256 devices in a mesh: expert: 8 (over z_lo, y), shard: 32 (over z_hi, x, core).
Axes of the slice: x: 4, y: 4, z: 8 (z_hi: 4, z_lo: 2; z = z_hi * 2 + z_lo), core: 2. Of those that a mesh axis runs over, the one named last changes fastest.
Arguments:
- tokens: bfloat16 [2048, 6144], P(('expert', 'shard')), may hold values from -6 to 6
- norm_gain: float32 [6144], replicated, may hold values from 0.5 to 1.5
- routes: int32 [2048, 2], P(('expert', 'shard')), may hold values from 0 to 7, all different within a row; in each aligned block of 8 rows (0 to 7, 8 to 15, ...) at most 4 rows name the same one
- gate_weights: float32 [2048, 2], P(('expert', 'shard')), may hold values from 0.2 to 1
- capacity: int32 [8], replicated, may hold values from 2 to 4
- w_gate: bfloat16 [8, 6144, 8192], P('expert', None, 'shard'), may hold values from -0.078125 to 0.078125
- w_up: bfloat16 [8, 6144, 8192], P('expert', None, 'shard'), may hold values from -0.078125 to 0.078125
- w_down: bfloat16 [8, 8192, 6144], P('expert', 'shard'), may hold values from -0.0625 to 0.0625
Outputs:
- mixed_out: bfloat16 [2048, 6144], P(('expert', 'shard'))
The draws below stay inside these ranges and needn't reach their ends.
Inputs may be any that keep to these rules, and one draw needn't show every extreme that they name: `routes`: each row names 2 different experts; among the rows of one device no expert is named by more than 4 rows.
All inputs are finite; a program needn't handle non-finite values.
Results may differ from the reference program's by a relative error of at most 0.019.
Values may be sent and summed in bfloat16 or wider, within the bound.
A program may use at most 128 MiB of HBM per device.

```python
import math
import jax
import jax.numpy as jnp
import numpy as np
from jax import lax

D = 6144
FF = 8192
TOPK = 2
TOK_DEV = 8
EXPERTS = 8
MOST = 4
TOKENS = 2048
N_SHARD = 32


def draw_capacity(key, part):
    drawn_caps = jax.random.randint(key, (EXPERTS,), MOST // 2, MOST + 1, dtype=jnp.int32)
    chosen = jax.random.randint(jax.random.fold_in(key, 7), (), 0, EXPERTS, dtype=jnp.int32)
    return jnp.where(jnp.arange(EXPERTS, dtype=jnp.int32) == chosen, MOST, drawn_caps).astype(jnp.int32)


def levels(rng, extent, shards, low, high):
    level, own = 1.0, jax.random.fold_in(rng, 6)
    for dim, blocks in shards:
        draws = jnp.exp(jax.random.uniform(jax.random.fold_in(own, dim), (blocks,), jnp.float32, low / len(shards), high / len(shards)))
        level = level * jnp.repeat(draws, extent[dim] // blocks).reshape([-1 if axis == dim else 1 for axis in range(len(extent))])
    return level


def assign_block(own_key, own, number, rows, amount, top, bound, skew):
    order = jax.random.permutation(own_key, amount)
    packed, usual = portions_of(amount, rows * top, bound, skew, True), portions_of(amount, rows * top, bound, skew, False)
    places = jnp.arange(amount)

    def named(tallies, offset_by):
        used = int((tallies > 0).sum())
        fixed = max(1, used // 4)
        passed = fixed + (places - fixed + offset_by * (used - fixed)) % max(1, amount - fixed)
        return jnp.zeros((amount,), jnp.int32).at[order[jnp.where(places < fixed, places, passed)]].set(jnp.asarray(tallies, jnp.int32))

    tallies = jnp.where(number % 4 == 0, named(packed, number // 4), named(usual, number - number // 4 - 1))
    mixed = jax.random.permutation(jax.random.fold_in(own, 3), amount)
    giver, sink = mixed[0:amount // 2 * 2:2], mixed[1:amount // 2 * 2:2]
    margin = jnp.minimum(tallies[giver] - 1, bound - tallies[sink]) // 2
    margin = jnp.where((giver == order[0]) | (sink == order[0]) | (tallies[sink] == 0), 0, jnp.maximum(margin, 0))
    passed = jax.random.randint(jax.random.fold_in(own, 4), (amount // 2,), 0, 1 << 20) % (margin + 1)
    tallies = tallies.at[giver].add(-passed).at[sink].add(passed)
    members = jnp.searchsorted(jnp.cumsum(tallies), jnp.arange(rows * top), side="right").astype(jnp.int32)
    listing = members.reshape(top, rows).T
    listing = listing[jax.random.permutation(jax.random.fold_in(own, 1), rows)]
    offset_by = jax.random.randint(jax.random.fold_in(own, 2), (rows, 1), 0, top)
    return jnp.take_along_axis(listing, (jnp.arange(top)[None, :] + offset_by) % top, axis=1)


def portions_of(amount, total, bound, lean, full):
    weights = [(1 << 20) // math.isqrt(standing ** lean) + 1 for standing in range(1, amount + 1)]
    largest = bound if full else min(bound, max(-(-total // amount), total * weights[0] // sum(weights)))
    least = 1 if total - largest >= amount - 1 else 0
    holding, surplus = [largest] + [least] * (amount - 1), total - largest - least * (amount - 1)
    while surplus > 0:
        free = [i for i in range(1, amount) if holding[i] < largest] or [i for i in range(1, amount) if holding[i] < bound]
        mass, budget = sum([weights[i] for i in free]), surplus
        for i in free:
            extra = min(bound - holding[i], max(1, budget * weights[i] // mass), surplus)
            holding[i] = holding[i] + extra
            surplus = surplus - extra
    return np.array(holding)


def centred(key, dims, scale, limit, cuts=(), held_as=jnp.bfloat16):
    gain = levels(key, dims, cuts, -0.22, 0.18) if cuts else 1.0
    result = jax.random.normal(key, dims, jnp.float32) * scale * gain
    return jnp.minimum(jnp.maximum(result, -limit), limit).astype(held_as)


def setup_inputs(seed: int = 0) -> dict:
    keys = jax.random.split(jax.random.key(seed), 9)
    tokens = centred(keys[0], (TOKENS, D), 1.0, 6.0, ((0, 256),))
    norm_gain = jnp.clip(1.0 + 0.1 * jax.random.normal(keys[1], (D,), jnp.float32), 0.5, 1.5)
    routes_keys = jax.random.split(jax.random.fold_in(keys[2], 1), TOKENS // TOK_DEV)
    routes_turns = jax.random.permutation(jax.random.fold_in(keys[2], 3), TOKENS // TOK_DEV)
    routes = jax.vmap(lambda own, number: assign_block(jax.random.fold_in(keys[2], 2), own, number, TOK_DEV, EXPERTS, TOPK, MOST, 2))(routes_keys, routes_turns).reshape((TOKENS, TOPK))
    gate_weights = jnp.clip(jnp.exp(math.log(1.0) - 1.609438 * jax.random.uniform(keys[3], (TOKENS, TOPK), jnp.float32) ** levels(keys[3], (TOKENS, TOPK), ((0, 256),), -0.2, 0.2)), 0.2, 1.0)
    capacity = draw_capacity(jax.random.fold_in(keys[8], 71), 0)
    w_gate = centred(keys[5], (EXPERTS, D, FF), D ** -0.5, 0.078125, ((0, 8), (2, 32)))
    w_up = centred(keys[6], (EXPERTS, D, FF), D ** -0.5, 0.078125, ((0, 8), (2, 32)))
    w_down = centred(keys[7], (EXPERTS, FF, D), FF ** -0.5, 0.0625, ((0, 8), (1, 32)))
    return {"tokens": tokens, "norm_gain": norm_gain, "routes": routes, "gate_weights": gate_weights, "capacity": capacity, "w_gate": w_gate, "w_up": w_up, "w_down": w_down}


def rms_norm(tokens, norm_gain):
    widened = tokens.astype(jnp.float32)
    mean_square = lax.optimization_barrier(jnp.mean(widened * widened, axis=-1, keepdims=True))
    return (widened * lax.rsqrt(mean_square + 1e-05) * norm_gain).astype(jnp.bfloat16)

def slot_ranks(blocked):
    equal_ids = blocked[:, :, None, :, None] == blocked[:, None, :, None, :]
    shared = jnp.any(equal_ids, axis=4).astype(jnp.int32)
    per_block = blocked.shape[1]
    positions = jnp.arange(per_block, dtype=jnp.int32)
    earlier = (positions[None, :] < positions[:, None]).astype(jnp.int32)
    return lax.optimization_barrier(jnp.sum(shared * earlier[None, :, :, None], axis=2)).astype(jnp.int32)

def expert_apply(buffer, gate_proj, up_proj, down_proj):
    gate_val = jnp.dot(buffer, gate_proj, preferred_element_type=jnp.float32)
    up_val = jnp.dot(buffer, up_proj, preferred_element_type=jnp.float32)
    hidden = (jax.nn.silu(gate_val) * up_val).astype(jnp.bfloat16)
    hidden_width = FF // N_SHARD

    def add_shard(running, shard_idx):
        start_col = (shard_idx * hidden_width).astype(jnp.int32)
        hidden_part = lax.dynamic_slice_in_dim(hidden, start_col, hidden_width, 1)
        down_part = lax.dynamic_slice_in_dim(down_proj, start_col, hidden_width, 0)
        rounded = jnp.dot(hidden_part, down_part, preferred_element_type=jnp.float32).astype(jnp.bfloat16)
        rounded = lax.optimization_barrier(rounded)
        return (running + rounded.astype(jnp.float32), None)
    initial = jnp.zeros((buffer.shape[0], down_proj.shape[1]), jnp.float32)
    running, _ = lax.scan(add_shard, initial, jnp.arange(N_SHARD, dtype=jnp.int32))
    return running.astype(jnp.bfloat16)

def reference(tokens, norm_gain, routes, gate_weights, capacity, w_gate, w_up, w_down):
    normed = rms_norm(tokens, norm_gain)
    nblocks = TOKENS // TOK_DEV
    slot_rank = slot_ranks(routes.reshape(nblocks, TOK_DEV, TOPK)).reshape(TOKENS, TOPK)
    kept_mask = slot_rank < capacity[routes]
    block_ids = (jnp.arange(TOKENS, dtype=jnp.int32) // TOK_DEV)[:, None]
    slot_index = (block_ids * MOST + slot_rank).astype(jnp.int32)
    dump_row = nblocks * MOST
    mixed_out = jnp.zeros((TOKENS, D), jnp.float32)
    for expert_idx in range(EXPERTS):
        routed_mask = kept_mask & (routes == expert_idx)
        dest_rows = jnp.where(routed_mask, slot_index, dump_row).astype(jnp.int32)
        buffer = jnp.zeros((dump_row + 1, D), jnp.bfloat16)
        for slot_k in range(TOPK):
            buffer = buffer.at[dest_rows[:, slot_k]].set(normed)
        expert_out = expert_apply(buffer, w_gate[expert_idx], w_up[expert_idx], w_down[expert_idx])
        for slot_k in range(TOPK):
            taken = expert_out[dest_rows[:, slot_k]].astype(jnp.float32)
            weighted = gate_weights[:, slot_k:slot_k + 1] * taken
            mixed_out = mixed_out + jnp.where(routed_mask[:, slot_k:slot_k + 1], weighted, jnp.float32(0.0))
    return mixed_out.astype(jnp.bfloat16)
```

```python
import jax
import jax.numpy as jnp
from jax import lax
from jax.experimental import pallas as pl
from jax.experimental.pallas import tpu as pltpu
from jax.sharding import PartitionSpec as P

MESH = pl.DeviceIdType.MESH
F32, BF16 = jnp.float32, jnp.bfloat16

D = 6144
HALF = D // 2
FW = 256
META = 128
CHUNKS = 4


def device_of(x, y, z, core):
    return (lax.rem(z, 2) * 4 + y, (z // 2) * 8 + x * 2 + core)


def remote(src, dst, send, recv, device):
    return pltpu.make_async_remote_copy(
        src_ref=src,
        dst_ref=dst,
        send_sem=send,
        recv_sem=recv,
        device_id=device,
        device_id_type=MESH,
    )


def routing_lanes(routes, gates, cap_ref):
    lane = lax.broadcasted_iota(jnp.int32, (8, META), 1)
    row = lax.broadcasted_iota(jnp.int32, (8, META), 0)
    expert, slot = lane // 4, lane % 4
    named = [routes[:, k : k + 1] == expert for k in range(2)]
    either = (named[0] | named[1]).astype(jnp.int32)
    running = either
    for shift in (1, 2, 4):
        running = running + jnp.where(row >= shift, pltpu.roll(running, shift, 0), 0)
    rank = running - either
    limit = jnp.zeros((8, META), jnp.int32)
    for e in range(8):
        limit = jnp.where(expert == e, cap_ref[e], limit)
    held = (rank == slot) & (rank < limit)
    weights = jnp.zeros((8, META), F32)
    for k in range(2):
        weights = weights + jnp.where(named[k] & held, gates[:, k : k + 1], 0.0)
    high = weights.astype(BF16).astype(F32)
    middle = (weights - high).astype(BF16).astype(F32)
    low = weights - high - middle
    return high + pltpu.roll(middle, 32, 1) + pltpu.roll(low, 64, 1)


def kernel(
    tok_ref, gain_ref, routes_ref, gates_ref, cap_ref, wg_ref, wu_ref, wd_ref, out_ref,
    pair_src, pair_dst, ztok, sbuf, xbuf, wgu, wdn, gsend, grecv, gown, hbuf,
    ybuf, r1buf, r2buf, rbuf, yret, zsend, zret, fin_src, fin_dst,
    pair_sem, z_s, z_r, y_s, y_r, x1_s, x1_r, x2_s, x2_r, w_l, w_s, w_r, g_s, g_r, h_s, h_r,
    r1_s, r1_r, r2_s, r2_r, yr_s, yr_r, zr_s, zr_r, fin_sem,
):
    me_e, me_s = lax.axis_index("expert"), lax.axis_index("shard")
    z_lo, y = me_e // 4, lax.rem(me_e, 4)
    z = (me_s // 8) * 2 + z_lo
    x = lax.rem(me_s // 2, 4)
    core = lax.rem(me_s, 2)
    sibling = device_of(x, y, z, 1 - core)
    left = device_of(lax.rem(x + 3, 4), y, z, core)
    right = device_of(lax.rem(x + 1, 4), y, z, core)

    def at_y(r):
        return device_of(x, lax.rem(y + r, 4), z, core)

    def at_z(d):
        return device_of(x, y, lax.rem(z + d, 8), core)

    place = {0: 0, 1: 1, 7: 2, 2: 3, 6: 4, 3: 5, 5: 6, 4: 7}

    mine = pl.ds(pl.multiple_of(core * HALF, HALF), HALF)
    other = pl.ds(pl.multiple_of((1 - core) * HALF, HALF), HALF)
    local_weights = [
        pltpu.make_async_copy(wg_ref.at[0, mine], wgu.at[2], w_l.at[0]),
        pltpu.make_async_copy(wu_ref.at[0, mine], wgu.at[3], w_l.at[1]),
        pltpu.make_async_copy(wd_ref.at[0, :, mine], wdn.at[0], w_l.at[2]),
    ]
    pair_weights = [
        remote(wg_ref.at[0, other], wgu.at[0], w_s.at[0], w_r.at[0], sibling),
        remote(wu_ref.at[0, other], wgu.at[1], w_s.at[1], w_r.at[1], sibling),
        remote(wd_ref.at[0, :, other], wdn.at[1], w_s.at[2], w_r.at[2], sibling),
    ]
    for copy in local_weights:
        copy.start()

    barrier = pltpu.get_barrier_semaphore()
    greeted = [sibling, left, right] + [at_y(r) for r in (1, 2, 3)] + [at_z(d) for d in range(1, 8)]
    for device in greeted:
        pl.semaphore_signal(barrier, inc=1, device_id=device, device_id_type=MESH)

    tokens = tok_ref[...].astype(F32)
    scale = lax.rsqrt(jnp.mean(tokens * tokens, axis=-1, keepdims=True) + 1e-05)
    normed = tokens * scale * gain_ref[...]
    lanes = routing_lanes(routes_ref[...], gates_ref[...], cap_ref)
    first = core == 0
    own_half = jnp.where(first, normed[:, :HALF], normed[:, HALF:])
    pair_src[:, :HALF] = jnp.where(first, normed[:, HALF:], normed[:, :HALF]).astype(BF16)
    pair_src[:, HALF:] = lanes.astype(BF16)

    pl.semaphore_wait(barrier, len(greeted))
    pair = remote(pair_src, pair_dst, pair_sem.at[0], pair_sem.at[1], sibling)
    pair.start()
    for copy in pair_weights:
        copy.start()
    pair.wait_recv()
    their_half = pair_dst[:, :HALF].astype(F32)
    their_lanes = pair_dst[:, HALF:].astype(F32)
    ztok[0, :, :HALF] = jnp.concatenate(
        [jnp.where(first, own_half, their_half), jnp.where(first, their_half, own_half)], axis=0
    ).astype(BF16)
    ztok[0, :, HALF:] = jnp.concatenate(
        [jnp.where(first, lanes, their_lanes), jnp.where(first, their_lanes, lanes)], axis=0
    ).astype(BF16)

    def z_copy(d):
        n = place[d]
        return remote(ztok.at[0], ztok.at[n], z_s.at[n], z_r.at[n], at_z(8 - d))

    for d in (1, 7, 2, 6, 3, 5, 4):
        z_copy(d).start()

    def z_arrival(n):
        return remote(ztok.at[0], ztok.at[n], z_s.at[n], z_r.at[n], at_z(1))

    def weights_of(k, turned):
        meta = ztok[pl.ds(2 * k, 2), :, HALF:].reshape(32, META)
        shape = (64, META) if turned else (META, 64)
        lane = lax.broadcasted_iota(jnp.int32, shape, 1 if turned else 0)
        column = lax.broadcasted_iota(jnp.int32, shape, 0 if turned else 1)
        expert = z_lo * 4 + (y + column // 16) % 4
        wanted = expert * 4 + column % 4
        pick = ((lane % 32 == wanted) & (lane < 96)).astype(F32).astype(BF16)
        if turned:
            raw = lax.dot_general(pick, meta, (((1,), (1,)), ((), ())), preferred_element_type=F32)
        else:
            raw = jnp.dot(meta, pick, preferred_element_type=F32)
        shape = (64, 32) if turned else (32, 64)
        column = lax.broadcasted_iota(jnp.int32, shape, 0 if turned else 1)
        row = lax.broadcasted_iota(jnp.int32, shape, 1 if turned else 0)
        return jnp.where(row // 8 == (column // 4) % 4, raw, 0.0)

    def y_copy(k, r):
        return remote(sbuf.at[k, r - 1], xbuf.at[k, 0, 4 - r], y_s.at[k, r - 1], y_r.at[k, 3 - r], at_y(r))

    def y_arrival(k, i):
        return remote(sbuf.at[k, 0], xbuf.at[k, 0, i], y_s.at[k, 0], y_r.at[k, i - 1], at_y(1))

    def dispatch(k):
        @pl.when(k > 0)
        def _():
            z_arrival(2 * k).wait_recv()

        z_arrival(2 * k + 1).wait_recv()
        picker = jnp.where(weights_of(k, True) != 0.0, 1.0, 0.0).astype(BF16)
        step = HALF // 4
        for n in range(4):
            columns = slice(n * step, (n + 1) * step)
            slab = ztok[pl.ds(2 * k, 2), :, columns].reshape(32, step)
            slots = jnp.dot(picker, slab, preferred_element_type=F32).astype(BF16).reshape(4, 16, step)
            xbuf[k, 0, 0, :, columns] = slots[0]
            sbuf[k, :, :, columns] = slots[1:]
        for r in (2, 1, 3):
            y_copy(k, r).start()

    def x1_copies(k):
        return (
            remote(xbuf.at[k, 0], xbuf.at[k, 1], x1_s.at[k, 0], x1_r.at[k, 0], right),
            remote(xbuf.at[k, 0], xbuf.at[k, 2], x1_s.at[k, 1], x1_r.at[k, 1], left),
        )

    def x2_copies(k):
        low, high = pl.ds(0, 2), pl.ds(2, 2)
        return (
            remote(xbuf.at[k, 1, low], xbuf.at[k, 3, low], x2_s.at[k, 0], x2_r.at[k, 0], right),
            remote(xbuf.at[k, 2, high], xbuf.at[k, 3, high], x2_s.at[k, 1], x2_r.at[k, 1], left),
        )

    def gather_near(k):
        for i in (1, 3, 2):
            y_arrival(k, i).wait_recv()
        for copy in x1_copies(k):
            copy.start()

    def gather_far(k):
        for near, far in zip(x1_copies(k), x2_copies(k)):
            near.wait_recv()
            far.start()

    def pre_activations(k):
        return remote(gsend.at[k], grecv.at[k], g_s.at[k], g_r.at[k], sibling)

    def hidden_copy(k):
        return remote(hbuf.at[k, 0], hbuf.at[k, 1], h_s.at[k], h_r.at[k], sibling)

    def r1_copies(k):
        low, high = pl.ds(0, 2), pl.ds(2, 2)
        return (
            remote(ybuf.at[k, 3, low], r1buf.at[k, 0], r1_s.at[k, 0], r1_r.at[k, 0], left),
            remote(ybuf.at[k, 3, high], r1buf.at[k, 1], r1_s.at[k, 1], r1_r.at[k, 1], right),
        )

    def r2_copies(k):
        return (
            remote(ybuf.at[k, 1], r2buf.at[k, 1], r2_s.at[k, 1], r2_r.at[k, 1], left),
            remote(ybuf.at[k, 2], r2buf.at[k, 0], r2_s.at[k, 0], r2_r.at[k, 0], right),
        )

    def expert_apply(k):
        @pl.when(k == 0)
        def _():
            for copy in local_weights:
                copy.wait()
            for copy in pair_weights:
                copy.wait_recv()

        for copy in x2_copies(k):
            copy.wait_recv()

        def project(n):
            rows = xbuf[k].reshape(256, HALF)
            return jnp.dot(rows, wgu[n], preferred_element_type=F32)

        @pl.loop(0, 2)
        def _(n):
            gsend[k, n] = project(n)

        pre_activations(k).start()

        @pl.loop(0, 2)
        def _(n):
            gown[n] = project(n + 2)

        pre_activations(k).wait_recv()
        gate = gown[0] + grecv[k, 0]
        up = gown[1] + grecv[k, 1]
        hbuf[k, 0] = (gate / (1.0 + jnp.exp(-gate)) * up).astype(BF16)
        hidden_copy(k).start()
        hidden_copy(k).wait_recv()
        step = 512

        @pl.loop(0, HALF // step)
        def _(n):
            columns = pl.ds(pl.multiple_of(n * step, step), step)
            made = jnp.dot(hbuf[k, 0], wdn[0, :, columns], preferred_element_type=F32)
            made = made + jnp.dot(hbuf[k, 1], wdn[1, :, columns], preferred_element_type=F32)
            ybuf[k, :, :, :, columns] = made.astype(BF16).reshape(4, 4, 16, step)

        for copy in r1_copies(k):
            copy.start()

    def return_near(k):
        for copy in r1_copies(k):
            copy.wait_recv()
        ybuf[k, 1, 0:2] = (ybuf[k, 1, 0:2].astype(F32) + r1buf[k, 0].astype(F32)).astype(BF16)
        ybuf[k, 2, 2:4] = (ybuf[k, 2, 2:4].astype(F32) + r1buf[k, 1].astype(F32)).astype(BF16)
        for copy in r2_copies(k):
            copy.start()

    def yr_copy(k, i):
        return remote(rbuf.at[k, i - 1], yret.at[k, 4 - i], yr_s.at[k, i - 1], yr_r.at[k, 3 - i], at_y(i))

    def yr_arrival(k, r):
        return remote(rbuf.at[k, 0], yret.at[k, r], yr_s.at[k, 0], yr_r.at[k, r - 1], at_y(1))

    def return_rows(k):
        for copy in r2_copies(k):
            copy.wait_recv()
        total = ybuf[k, 0].astype(F32) + r2buf[k, 0].astype(F32) + r2buf[k, 1].astype(F32)
        total = total.astype(BF16)
        yret[k, 0] = total[0]
        rbuf[k] = total[1:]
        for i in (2, 1, 3):
            yr_copy(k, i).start()

    def zr_copy(n, d):
        return remote(zsend.at[n], zret.at[n], zr_s.at[n], zr_r.at[n], at_z(d))

    def combine(k):
        for r in (1, 3, 2):
            yr_arrival(k, r).wait_recv()
        weights = weights_of(k, False)
        high = weights.astype(BF16)
        rest = (weights - high.astype(F32)).astype(BF16)
        step = HALF // 4
        for n in range(4):
            columns = slice(n * step, (n + 1) * step)
            rows = yret[k, :, :, columns].reshape(64, step)
            made = jnp.dot(high, rows, preferred_element_type=F32)
            made = made + jnp.dot(rest, rows, preferred_element_type=F32)
            zsend[pl.ds(2 * k, 2), :, columns] = made.astype(BF16).reshape(2, 16, step)

        @pl.when(k > 0)
        def _():
            zr_copy(2 * k, 8 - k).start()

        zr_copy(2 * k + 1, k + 1).start()

    def when(k, work):
        @pl.when((k >= 0) & (k < CHUNKS))
        def _():
            work(k)

    dispatch(0)

    def step_of(t, carry):
        when(t - 5, combine)
        when(t, gather_near)
        when(t + 1, dispatch)
        when(t - 1, gather_far)
        when(t - 4, return_rows)
        when(t - 3, return_near)
        when(t - 2, expert_apply)
        return carry

    lax.fori_loop(0, CHUNKS + 5, step_of, 0)

    total = zsend[0].astype(F32)
    for n in range(1, 8):
        zr_copy(n, 1).wait_recv()
        total = total + zret[n].astype(F32)
    total = total.astype(BF16).astype(F32)
    fin_src[...] = jnp.where(first, total[8:], total[:8]).astype(BF16)
    fin = remote(fin_src, fin_dst, fin_sem.at[0], fin_sem.at[1], sibling)
    fin.start()
    kept = jnp.where(first, total[:8], total[8:])
    fin.wait_recv()
    theirs = fin_dst[...].astype(F32)
    out_ref[:, :HALF] = jnp.where(first, kept, theirs).astype(BF16)
    out_ref[:, HALF:] = jnp.where(first, theirs, kept).astype(BF16)

    fin.wait_send()
    pair.wait_send()
    for copy in pair_weights:
        copy.wait_send()
    for d in range(1, 8):
        z_copy(d).wait_send()
        zr_copy(d, 1).wait_send()

    def sent(k, carry):
        for r in (1, 2, 3):
            y_copy(k, r).wait_send()
            yr_copy(k, r).wait_send()
        for copy in x1_copies(k) + x2_copies(k) + r1_copies(k) + r2_copies(k):
            copy.wait_send()
        pre_activations(k).wait_send()
        hidden_copy(k).wait_send()
        return carry

    lax.fori_loop(0, CHUNKS, sent, 0)


def on_device(tokens, norm_gain, routes, gate_weights, capacity, w_gate, w_up, w_down):
    vmem, smem = pl.BlockSpec(memory_space=pltpu.VMEM), pl.BlockSpec(memory_space=pltpu.SMEM)
    whole = pl.BlockSpec(memory_space=pl.ANY)
    sems = pltpu.SemaphoreType.DMA
    k = CHUNKS
    return pl.pallas_call(
        kernel,
        out_shape=jax.ShapeDtypeStruct((8, D), BF16),
        in_specs=[vmem, vmem, vmem, vmem, smem, whole, whole, whole],
        out_specs=vmem,
        scratch_shapes=[
            pltpu.VMEM((8, HALF + META), BF16),
            pltpu.VMEM((8, HALF + META), BF16),
            pltpu.VMEM((8, 16, HALF + META), BF16),
            pltpu.VMEM((k, 3, 16, HALF), BF16),
            pltpu.VMEM((k, 4, 4, 16, HALF), BF16),
            pltpu.VMEM((4, HALF, FW), BF16),
            pltpu.VMEM((2, FW, HALF), BF16),
            pltpu.VMEM((k, 2, 256, FW), F32),
            pltpu.VMEM((k, 2, 256, FW), F32),
            pltpu.VMEM((2, 256, FW), F32),
            pltpu.VMEM((k, 2, 256, FW), BF16),
            pltpu.VMEM((k, 4, 4, 16, HALF), BF16),
            pltpu.VMEM((k, 2, 2, 16, HALF), BF16),
            pltpu.VMEM((k, 2, 4, 16, HALF), BF16),
            pltpu.VMEM((k, 3, 16, HALF), BF16),
            pltpu.VMEM((k, 4, 16, HALF), BF16),
            pltpu.VMEM((8, 16, HALF), BF16),
            pltpu.VMEM((8, 16, HALF), BF16),
            pltpu.VMEM((8, HALF), BF16),
            pltpu.VMEM((8, HALF), BF16),
            sems((2,)),
            sems((8,)), sems((8,)),
            sems((k, 3)), sems((k, 3)),
            sems((k, 2)), sems((k, 2)),
            sems((k, 2)), sems((k, 2)),
            sems((3,)), sems((3,)), sems((3,)),
            sems((k,)), sems((k,)),
            sems((k,)), sems((k,)),
            sems((k, 2)), sems((k, 2)),
            sems((k, 2)), sems((k, 2)),
            sems((k, 3)), sems((k, 3)),
            sems((8,)), sems((8,)),
            sems((2,)),
        ],
        compiler_params=pltpu.CompilerParams(
            collective_id=0, has_side_effects=True, vmem_limit_bytes=67043328
        ),
    )(tokens, norm_gain[None], routes, gate_weights, capacity, w_gate, w_up, w_down)


def solution(mesh):
    in_specs = (
        P(("expert", "shard"), None),
        P(),
        P(("expert", "shard"), None),
        P(("expert", "shard"), None),
        P(),
        P("expert", None, "shard"),
        P("expert", None, "shard"),
        P("expert", "shard", None),
    )
    out_specs = P(("expert", "shard"), None)
    return jax.shard_map(
        on_device, mesh=mesh, in_specs=in_specs, out_specs=out_specs, check_vma=False
    )
```

```python
import jax
import jax.numpy as jnp
from jax import lax
from jax.experimental import pallas as pl
from jax.experimental.pallas import tpu as pltpu
from jax.sharding import PartitionSpec as P

MESH = pl.DeviceIdType.MESH
F32, BF16 = jnp.float32, jnp.bfloat16

D = 6144
HALF = D // 2
FW = 256
META = 128
CHUNKS = 4
A = 1792
B = HALF - A
TILE = 256


def device_of(x, y, z, core):
    return (lax.rem(z, 2) * 4 + y, (z // 2) * 8 + x * 2 + core)


def remote(src, dst, send, recv, device):
    return pltpu.make_async_remote_copy(
        src_ref=src,
        dst_ref=dst,
        send_sem=send,
        recv_sem=recv,
        device_id=device,
        device_id_type=MESH,
    )


def columns_of(pair):
    row = lax.broadcasted_iota(jnp.int32, (8, 8), 0)
    lane = lax.broadcasted_iota(jnp.int32, (8, 8), 1)
    spread = [jnp.broadcast_to(pair[k : k + 1, :], (8, 8)) for k in range(2)]
    zero = jnp.zeros((8, 8), pair.dtype)
    return [jnp.sum(jnp.where(row == lane, s, zero), axis=1, keepdims=True) for s in spread]


def routing_lanes(routes, gates, cap_ref):
    lane = lax.broadcasted_iota(jnp.int32, (8, META), 1)
    row = lax.broadcasted_iota(jnp.int32, (8, META), 0)
    expert, slot = lane // 4, lane % 4
    named = [routes[k] == expert for k in range(2)]
    either = (named[0] | named[1]).astype(jnp.int32)
    running = either
    for shift in (1, 2, 4):
        running = running + jnp.where(row >= shift, pltpu.roll(running, shift, 0), 0)
    rank = running - either
    limit = jnp.zeros((8, META), jnp.int32)
    for e in range(8):
        limit = jnp.where(expert == e, cap_ref[e], limit)
    held = (rank == slot) & (rank < limit)
    weights = jnp.zeros((8, META), F32)
    for k in range(2):
        weights = weights + jnp.where(named[k] & held, gates[k], 0.0)
    high = weights.astype(BF16).astype(F32)
    middle = (weights - high).astype(BF16).astype(F32)
    low = weights - high - middle
    return high + pltpu.roll(middle, 32, 1) + pltpu.roll(low, 64, 1)


def kernel(
    tok_ref, gain_ref, routes_ref, gates_ref, cap_ref, wg_ref, wu_ref, wd_ref, out_ref,
    pair_src, pair_dst, ztok, sbuf_a, sbuf_b, xtok, xbuf_a, xbuf_b, wgu, wdn, gsend, grecv, gown, hbuf,
    ybuf_a, ybuf_b, r1buf, r2buf, rbuf, yret_a, yret_b, tokb, t1buf, t2buf, zsend, zret, fin_src, fin_dst,
    pair_sem, z_s, z_r, ya_s, ya_r, yb_s, yb_r, x1_s, x1_r, x2_s, x2_r, b1_s, b1_r, b2_s, b2_r,
    w_l, w_s, w_r, g_s, g_r, h_s, h_r, r1_s, r1_r, r2_s, r2_r, t1_s, t1_r, t2_s, t2_r,
    yra_s, yra_r, yrb_s, yrb_r, zr_s, zr_r, fin_sem,
):
    me_e, me_s = lax.axis_index("expert"), lax.axis_index("shard")
    z_lo, y = me_e // 4, lax.rem(me_e, 4)
    z = (me_s // 8) * 2 + z_lo
    x = lax.rem(me_s // 2, 4)
    core = lax.rem(me_s, 2)
    sibling = device_of(x, y, z, 1 - core)
    left = device_of(lax.rem(x + 3, 4), y, z, core)
    right = device_of(lax.rem(x + 1, 4), y, z, core)

    def at_y(r):
        return device_of(x, lax.rem(y + r, 4), z, core)

    def at_z(d):
        return device_of(x, y, lax.rem(z + d, 8), core)

    barrier = pltpu.get_barrier_semaphore()
    greeted = [at_z(d) for d in (4, 3, 5, 2, 6, 1, 7)] + [at_y(r) for r in (2, 1, 3)] + [left, right, sibling]
    for device in greeted:
        pl.semaphore_signal(barrier, inc=1, device_id=device, device_id_type=MESH)

    own = 1

    def place(d):
        return d - 1 if d % 2 else (8 - d) % 8 + 1

    mine = pl.ds(pl.multiple_of(core * HALF, HALF), HALF)
    other = pl.ds(pl.multiple_of((1 - core) * HALF, HALF), HALF)
    local_weights = [
        pltpu.make_async_copy(wg_ref.at[0, mine], wgu.at[2], w_l.at[0]),
        pltpu.make_async_copy(wu_ref.at[0, mine], wgu.at[3], w_l.at[1]),
        pltpu.make_async_copy(wd_ref.at[0, :, mine], wdn.at[0], w_l.at[2]),
    ]
    pair_weights = [
        remote(wg_ref.at[0, other], wgu.at[0], w_s.at[0], w_r.at[0], sibling),
        remote(wu_ref.at[0, other], wgu.at[1], w_s.at[1], w_r.at[1], sibling),
        remote(wd_ref.at[0, :, other], wdn.at[1], w_s.at[2], w_r.at[2], sibling),
    ]
    for copy in local_weights:
        copy.start()

    tokens = tok_ref[...].astype(F32)
    scale = lax.rsqrt(jnp.mean(tokens * tokens, axis=-1, keepdims=True) + 1e-05)
    normed = tokens * scale * gain_ref[...]
    lanes = routing_lanes(columns_of(routes_ref[...]), columns_of(gates_ref[...]), cap_ref)
    first = core == 0
    own_half = jnp.where(first, normed[:, :HALF], normed[:, HALF:])
    pair_src[:, :HALF] = jnp.where(first, normed[:, HALF:], normed[:, :HALF]).astype(BF16)
    pair_src[:, HALF:] = lanes.astype(BF16)

    pl.semaphore_wait(barrier, len(greeted))
    pair = remote(pair_src, pair_dst, pair_sem.at[0], pair_sem.at[1], sibling)
    pair.start()
    for copy in pair_weights:
        copy.start()
    pair.wait_recv()
    their_half = pair_dst[:, :HALF].astype(F32)
    their_lanes = pair_dst[:, HALF:].astype(F32)
    ztok[own, :, :HALF] = jnp.concatenate(
        [jnp.where(first, own_half, their_half), jnp.where(first, their_half, own_half)], axis=0
    ).astype(BF16)
    ztok[own, :, HALF:] = jnp.concatenate(
        [jnp.where(first, lanes, their_lanes), jnp.where(first, their_lanes, lanes)], axis=0
    ).astype(BF16)

    def z_copy(d):
        n = place(d)
        return remote(ztok.at[own], ztok.at[n], z_s.at[n], z_r.at[n], at_z(8 - d))

    for d in (1, 3, 6, 5, 4, 7, 2):
        z_copy(d).start()

    def z_arrival(n):
        return remote(ztok.at[own], ztok.at[n], z_s.at[n], z_r.at[n], at_z(1))

    def weights_of(meta, turned):
        shape = (64, META) if turned else (META, 64)
        lane = lax.broadcasted_iota(jnp.int32, shape, 1 if turned else 0)
        column = lax.broadcasted_iota(jnp.int32, shape, 0 if turned else 1)
        expert = z_lo * 4 + (y + column // 16) % 4
        wanted = expert * 4 + column % 4
        pick = ((lane % 32 == wanted) & (lane < 96)).astype(F32).astype(BF16)
        if turned:
            raw = lax.dot_general(pick, meta, (((1,), (1,)), ((), ())), preferred_element_type=F32)
        else:
            raw = jnp.dot(meta, pick, preferred_element_type=F32)
        shape = (64, 32) if turned else (32, 64)
        column = lax.broadcasted_iota(jnp.int32, shape, 0 if turned else 1)
        row = lax.broadcasted_iota(jnp.int32, shape, 1 if turned else 0)
        return jnp.where(row // 8 == (column // 4) % 4, raw, 0.0)

    def picker_of(meta):
        return jnp.where(weights_of(meta, True) != 0.0, 1.0, 0.0).astype(BF16)

    def picked(picker, slab):
        return jnp.dot(picker, slab, preferred_element_type=F32).astype(BF16).reshape(4, 16, slab.shape[1])

    def combined(weights, rows):
        high = weights.astype(BF16)
        rest = (weights - high.astype(F32)).astype(BF16)
        made = jnp.dot(high, rows, preferred_element_type=F32) + jnp.dot(rest, rows, preferred_element_type=F32)
        return made.astype(BF16).reshape(2, 16, rows.shape[1])

    def ya_copy(k, r):
        return remote(sbuf_a.at[k, r - 1], xbuf_a.at[k, 0, 4 - r], ya_s.at[k, r - 1], ya_r.at[k, 3 - r], at_y(r))

    PARTS = ((0, 1), (1, 2), (3, 1))

    def yb_copy(k, part, r):
        rows = pl.ds(*PARTS[part])
        return remote(
            sbuf_b.at[k, r - 1, rows], xbuf_b.at[k, rows, 4 - r], yb_s.at[k, part, r - 1], yb_r.at[k, part, 3 - r], at_y(r)
        )

    def x1_copies(k):
        return (
            remote(xbuf_a.at[k, 0], xbuf_a.at[k, 1], x1_s.at[k, 0], x1_r.at[k, 0], right),
            remote(xbuf_a.at[k, 0], xbuf_a.at[k, 2], x1_s.at[k, 1], x1_r.at[k, 1], left),
        )

    def x2_copies(k):
        low, high = pl.ds(0, 2), pl.ds(2, 2)
        return (
            remote(xbuf_a.at[k, 1, low], xbuf_a.at[k, 3, low], x2_s.at[k, 0], x2_r.at[k, 0], right),
            remote(xbuf_a.at[k, 2, high], xbuf_a.at[k, 3, high], x2_s.at[k, 1], x2_r.at[k, 1], left),
        )

    def b1_copies(k):
        source = ztok.at[pl.ds(2 * k, 2), :, A:]
        return (
            remote(source, xtok.at[k, 0], b1_s.at[k, 0], b1_r.at[k, 0], right),
            remote(source, xtok.at[k, 1], b1_s.at[k, 1], b1_r.at[k, 1], left),
        )

    def b2_copies(k):
        return (
            remote(xtok.at[k, 0, 0], xtok.at[k, 2, 0], b2_s.at[k, 0], b2_r.at[k, 0], right),
            remote(xtok.at[k, 1, 1], xtok.at[k, 2, 1], b2_s.at[k, 1], b2_r.at[k, 1], left),
        )

    def dispatch(k):
        z_arrival(2 * k).wait_recv()

        @pl.when(k > 0)
        def _():
            z_arrival(2 * k + 1).wait_recv()

        for copy in b1_copies(k):
            copy.start()
        picker = picker_of(ztok[pl.ds(2 * k, 2), :, HALF:].reshape(32, META))

        def slots_at(start):
            return picked(picker, ztok[pl.ds(2 * k, 2), :, start : start + TILE].reshape(32, TILE))

        for start in range(0, A, TILE):
            slots = slots_at(start)
            xbuf_a[k, 0, 0, :, start : start + TILE] = slots[0]
            sbuf_a[k, :, :, start : start + TILE] = slots[1:]
        for r in (2, 1, 3):
            ya_copy(k, r).start()
        for start in range(0, B, TILE):
            slots = slots_at(A + start)
            xbuf_b[k, 0, 0, :, start : start + TILE] = slots[0]
            sbuf_b[k, :, 0, :, start : start + TILE] = slots[1:]
        for r in (2, 1, 3):
            yb_copy(k, 0, r).start()

    def dispatch_from(k, rel):
        picker = picker_of(xtok[k, rel - 1, :, :, B:].reshape(32, META))
        for start in range(0, B, TILE):
            slots = picked(picker, xtok[k, rel - 1, :, :, start : start + TILE].reshape(32, TILE))
            xbuf_b[k, rel, 0, :, start : start + TILE] = slots[0]
            sbuf_b[k, :, rel, :, start : start + TILE] = slots[1:]

    def gather_near(k):
        for near, far in zip(b1_copies(k), b2_copies(k)):
            near.wait_recv()
            far.start()
        for r in (1, 3, 2):
            ya_copy(k, r).wait_recv()
        for copy in x1_copies(k):
            copy.start()

        @pl.loop(1, 3)
        def _(rel):
            dispatch_from(k, rel)

        for r in (2, 1, 3):
            yb_copy(k, 1, r).start()

    def gather_far(k):
        for copy in b2_copies(k):
            copy.wait_recv()
        dispatch_from(k, 3)
        for r in (2, 1, 3):
            yb_copy(k, 2, r).start()
        for near, far in zip(x1_copies(k), x2_copies(k)):
            near.wait_recv()
            far.start()

    def pre_activations(k):
        return remote(gsend.at[k], grecv.at[k], g_s.at[k], g_r.at[k], sibling)

    def hidden_copy(k):
        return remote(hbuf.at[k, 0], hbuf.at[k, 1], h_s.at[k], h_r.at[k], sibling)

    def r1_copies(k):
        low, high = pl.ds(0, 2), pl.ds(2, 2)
        return (
            remote(ybuf_a.at[k, 3, low], r1buf.at[k, 0], r1_s.at[k, 0], r1_r.at[k, 0], left),
            remote(ybuf_a.at[k, 3, high], r1buf.at[k, 1], r1_s.at[k, 1], r1_r.at[k, 1], right),
        )

    def r2_copies(k):
        return (
            remote(ybuf_a.at[k, 1], r2buf.at[k, 1], r2_s.at[k, 1], r2_r.at[k, 1], left),
            remote(ybuf_a.at[k, 2], r2buf.at[k, 0], r2_s.at[k, 0], r2_r.at[k, 0], right),
        )

    def yra_copy(k, i):
        return remote(rbuf.at[k, i - 1], yret_a.at[k, 4 - i], yra_s.at[k, i - 1], yra_r.at[k, 3 - i], at_y(i))

    def yrb_copy(k, i):
        return remote(ybuf_b.at[k, :, i], yret_b.at[k, :, 3 - i], yrb_s.at[k, i - 1], yrb_r.at[k, 3 - i], at_y(i))

    def t1_copies(k):
        return (
            remote(tokb.at[k, 3, 0], t1buf.at[k, 0], t1_s.at[k, 0], t1_r.at[k, 0], left),
            remote(tokb.at[k, 3, 1], t1buf.at[k, 1], t1_s.at[k, 1], t1_r.at[k, 1], right),
        )

    def t2_copies(k):
        return (
            remote(tokb.at[k, 1], t2buf.at[k, 1], t2_s.at[k, 1], t2_r.at[k, 1], left),
            remote(tokb.at[k, 2], t2buf.at[k, 0], t2_s.at[k, 0], t2_r.at[k, 0], right),
        )

    def expert_apply(k):
        @pl.when(k == 0)
        def _():
            for copy in local_weights:
                copy.wait()
            for copy in pair_weights:
                copy.wait_recv()

        for copy in x2_copies(k):
            copy.wait_recv()
        for part in range(3):
            for r in (1, 3, 2):
                yb_copy(k, part, r).wait_recv()

        def project(n):
            made = jnp.dot(xbuf_a[k].reshape(256, A), wgu[n, :A], preferred_element_type=F32)
            return made + jnp.dot(xbuf_b[k].reshape(256, B), wgu[n, A:], preferred_element_type=F32)

        @pl.loop(0, 2)
        def _(n):
            gsend[k, n] = project(n)

        pre_activations(k).start()

        @pl.loop(0, 2)
        def _(n):
            gown[n] = project(n + 2)

        pre_activations(k).wait_recv()
        gate = gown[0] + grecv[k, 0]
        up = gown[1] + grecv[k, 1]
        hbuf[k, 0] = (gate / (1.0 + jnp.exp(-gate)) * up).astype(BF16)
        hidden_copy(k).start()
        hidden_copy(k).wait_recv()

        def outputs(columns):
            made = jnp.dot(hbuf[k, 0], wdn[0, :, columns], preferred_element_type=F32)
            made = made + jnp.dot(hbuf[k, 1], wdn[1, :, columns], preferred_element_type=F32)
            return made.astype(BF16).reshape(4, 4, 16, TILE)

        @pl.loop(0, B // TILE)
        def _(n):
            start = pl.multiple_of(n * TILE, TILE)
            ybuf_b[k, :, :, :, pl.ds(start, TILE)] = outputs(pl.ds(pl.multiple_of(A + start, TILE), TILE))

        for i in (2, 1, 3):
            yrb_copy(k, i).start()

        @pl.loop(0, A // TILE)
        def _(n):
            start = pl.multiple_of(n * TILE, TILE)
            ybuf_a[k, :, :, :, pl.ds(start, TILE)] = outputs(pl.ds(start, TILE))

        for copy in r1_copies(k):
            copy.start()

    def plus(ref, *others):
        total = ref[...].astype(F32)
        for term in others:
            total = total + term[...].astype(F32)
        return total.astype(BF16)

    def return_near(k):
        for copy in r1_copies(k):
            copy.wait_recv()
        ybuf_a[k, 1, 0:2] = plus(ybuf_a.at[k, 1, 0:2], r1buf.at[k, 0])
        ybuf_a[k, 2, 2:4] = plus(ybuf_a.at[k, 2, 2:4], r1buf.at[k, 1])
        for copy in r2_copies(k):
            copy.start()
        for i in (1, 3, 2):
            yrb_copy(k, i).wait_recv()

        def combine_for(rel, meta):
            weights = weights_of(meta.reshape(32, META), False)
            for start in range(0, B, TILE):
                columns = slice(start, start + TILE)
                rows = jnp.concatenate([ybuf_b[k, rel, 0, :, columns][None], yret_b[k, rel, :, :, columns]], axis=0)
                tokb[k, rel, :, :, columns] = combined(weights, rows.reshape(64, TILE))

        combine_for(3, xtok[k, 2, :, :, B:])
        for copy in t1_copies(k):
            copy.start()
        combine_for(0, ztok[pl.ds(2 * k, 2), :, HALF:])

        @pl.loop(1, 3)
        def _(rel):
            combine_for(rel, xtok[k, rel - 1, :, :, B:])

    def return_rows(k):
        for copy in t1_copies(k):
            copy.wait_recv()
        tokb[k, 1, 0] = plus(tokb.at[k, 1, 0], t1buf.at[k, 0])
        tokb[k, 2, 1] = plus(tokb.at[k, 2, 1], t1buf.at[k, 1])
        for copy in t2_copies(k):
            copy.start()
        for copy in r2_copies(k):
            copy.wait_recv()
        total = plus(ybuf_a.at[k, 0], r2buf.at[k, 0], r2buf.at[k, 1])
        yret_a[k, 0] = total[0]
        rbuf[k] = total[1:]
        for i in (2, 1, 3):
            yra_copy(k, i).start()

    def zr_copy(n, d):
        return remote(zsend.at[n], zret.at[n], zr_s.at[n], zr_r.at[n], at_z(d))

    def combine(k):
        for copy in t2_copies(k):
            copy.wait_recv()
        zsend[pl.ds(2 * k, 2), :, A:] = plus(tokb.at[k, 0], t2buf.at[k, 0], t2buf.at[k, 1])
        for r in (1, 3, 2):
            yra_copy(k, r).wait_recv()
        weights = weights_of(ztok[pl.ds(2 * k, 2), :, HALF:].reshape(32, META), False)
        for start in range(0, A, TILE):
            columns = slice(start, start + TILE)
            zsend[pl.ds(2 * k, 2), :, columns] = combined(weights, yret_a[k, :, :, columns].reshape(64, TILE))
        zr_copy(2 * k, 2 * k + 1).start()

        @pl.when(k > 0)
        def _():
            zr_copy(2 * k + 1, 8 - 2 * k).start()

    def when(k, work):
        @pl.when((k >= 0) & (k < CHUNKS))
        def _():
            work(k)

    dispatch(0)

    def step_of(t, carry):
        when(t - 5, combine)
        when(t, gather_near)
        when(t + 1, dispatch)
        when(t - 1, gather_far)
        when(t - 4, return_rows)
        when(t - 3, return_near)
        when(t - 2, expert_apply)
        return carry

    lax.fori_loop(0, CHUNKS + 5, step_of, 0)

    total = zsend[own].astype(F32)
    for n in (0, 2, 3, 4, 5, 6, 7):
        zr_copy(n, 1).wait_recv()
        total = total + zret[n].astype(F32)
    total = total.astype(BF16).astype(F32)
    fin_src[...] = jnp.where(first, total[8:], total[:8]).astype(BF16)
    fin = remote(fin_src, fin_dst, fin_sem.at[0], fin_sem.at[1], sibling)
    fin.start()
    kept = jnp.where(first, total[:8], total[8:])
    fin.wait_recv()
    theirs = fin_dst[...].astype(F32)
    out_ref[:, :HALF] = jnp.where(first, kept, theirs).astype(BF16)
    out_ref[:, HALF:] = jnp.where(first, theirs, kept).astype(BF16)

    fin.wait_send()
    pair.wait_send()
    for copy in pair_weights:
        copy.wait_send()
    for d in range(1, 8):
        z_copy(d).wait_send()
    for n in (0, 2, 3, 4, 5, 6, 7):
        zr_copy(n, 1).wait_send()

    def sent(k, carry):
        for r in (1, 2, 3):
            ya_copy(k, r).wait_send()
            yra_copy(k, r).wait_send()
            yrb_copy(k, r).wait_send()
            for part in range(3):
                yb_copy(k, part, r).wait_send()
        for copies in (x1_copies, x2_copies, b1_copies, b2_copies, r1_copies, r2_copies, t1_copies, t2_copies):
            for copy in copies(k):
                copy.wait_send()
        pre_activations(k).wait_send()
        hidden_copy(k).wait_send()
        return carry

    lax.fori_loop(0, CHUNKS, sent, 0)


def on_device(tokens, norm_gain, routes, gate_weights, capacity, w_gate, w_up, w_down):
    vmem, smem = pl.BlockSpec(memory_space=pltpu.VMEM), pl.BlockSpec(memory_space=pltpu.SMEM)
    whole = pl.BlockSpec(memory_space=pl.ANY)
    k = CHUNKS

    def held(*shape, dtype=BF16):
        return pltpu.VMEM(shape, dtype)

    def sems(*shape):
        return [pltpu.SemaphoreType.DMA(shape)]

    return pl.pallas_call(
        kernel,
        out_shape=jax.ShapeDtypeStruct((8, D), BF16),
        in_specs=[vmem, vmem, vmem, vmem, smem, whole, whole, whole],
        out_specs=vmem,
        scratch_shapes=[
            held(8, HALF + META),
            held(8, HALF + META),
            held(8, 16, HALF + META),
            held(k, 3, 16, A),
            held(k, 3, 4, 16, B),
            held(k, 3, 2, 16, B + META),
            held(k, 4, 4, 16, A),
            held(k, 4, 4, 16, B),
            held(4, HALF, FW),
            held(2, FW, HALF),
            held(k, 2, 256, FW, dtype=F32),
            held(k, 2, 256, FW, dtype=F32),
            held(2, 256, FW, dtype=F32),
            held(k, 2, 256, FW),
            held(k, 4, 4, 16, A),
            held(k, 4, 4, 16, B),
            held(k, 2, 2, 16, A),
            held(k, 2, 4, 16, A),
            held(k, 3, 16, A),
            held(k, 4, 16, A),
            held(k, 4, 3, 16, B),
            held(k, 4, 2, 16, B),
            held(k, 2, 16, B),
            held(k, 2, 2, 16, B),
            held(8, 16, HALF),
            held(8, 16, HALF),
            held(8, HALF),
            held(8, HALF),
        ]
        + sems(2)
        + sems(8) * 2
        + sems(k, 3) * 2
        + sems(k, 3, 3) * 2
        + sems(k, 2) * 8
        + sems(3) * 3
        + sems(k) * 4
        + sems(k, 2) * 8
        + sems(k, 3) * 4
        + sems(8) * 2
        + sems(2),
        compiler_params=pltpu.CompilerParams(
            collective_id=0, has_side_effects=True, vmem_limit_bytes=67043328
        ),
    )(tokens, norm_gain[None], routes.T, gate_weights.T, capacity, w_gate, w_up, w_down)


def solution(mesh):
    in_specs = (
        P(("expert", "shard"), None),
        P(),
        P(("expert", "shard"), None),
        P(("expert", "shard"), None),
        P(),
        P("expert", None, "shard"),
        P("expert", None, "shard"),
        P("expert", "shard", None),
    )
    out_specs = P(("expert", "shard"), None)
    return jax.shard_map(
        on_device, mesh=mesh, in_specs=in_specs, out_specs=out_specs, check_vma=False
    )
```

```python
import jax
import jax.numpy as jnp
from jax import lax
from jax.experimental import pallas as pl
from jax.experimental.pallas import tpu as pltpu
from jax.sharding import PartitionSpec as P

MESH = pl.DeviceIdType.MESH
F32, BF16 = jnp.float32, jnp.bfloat16

D = 6144
HALF = D // 2
FW = 256
META = 128
CHUNKS = 4
A = 1792
B = HALF - A
TILE = 256


def device_of(x, y, z, core):
    return (lax.rem(z, 2) * 4 + y, (z // 2) * 8 + x * 2 + core)


def remote(src, dst, send, recv, device):
    return pltpu.make_async_remote_copy(
        src_ref=src,
        dst_ref=dst,
        send_sem=send,
        recv_sem=recv,
        device_id=device,
        device_id_type=MESH,
    )


def columns_of(pair):
    row = lax.broadcasted_iota(jnp.int32, (8, 8), 0)
    lane = lax.broadcasted_iota(jnp.int32, (8, 8), 1)
    spread = [jnp.broadcast_to(pair[k : k + 1, :], (8, 8)) for k in range(2)]
    zero = jnp.zeros((8, 8), pair.dtype)
    return [jnp.sum(jnp.where(row == lane, s, zero), axis=1, keepdims=True) for s in spread]


def routing_lanes(routes, gates, cap_ref):
    lane = lax.broadcasted_iota(jnp.int32, (8, META), 1)
    row = lax.broadcasted_iota(jnp.int32, (8, META), 0)
    expert, slot = lane // 4, lane % 4
    named = [routes[k] == expert for k in range(2)]
    either = (named[0] | named[1]).astype(jnp.int32)
    running = either
    for shift in (1, 2, 4):
        running = running + jnp.where(row >= shift, pltpu.roll(running, shift, 0), 0)
    rank = running - either
    limit = jnp.zeros((8, META), jnp.int32)
    for e in range(8):
        limit = jnp.where(expert == e, cap_ref[e], limit)
    held = (rank == slot) & (rank < limit)
    weights = jnp.zeros((8, META), F32)
    for k in range(2):
        weights = weights + jnp.where(named[k] & held, gates[k], 0.0)
    high = weights.astype(BF16).astype(F32)
    middle = (weights - high).astype(BF16).astype(F32)
    low = weights - high - middle
    return high + pltpu.roll(middle, 32, 1) + pltpu.roll(low, 64, 1)


def kernel(
    tok_ref, gain_ref, routes_ref, gates_ref, cap_ref, wg_ref, wu_ref, wd_ref, out_ref,
    pair_src, pair_dst, ztok, sbuf_a, sbuf_b, xtok, xbuf_a, xbuf_b, wgu, wdn, gsend, grecv, gown, hbuf,
    ybuf_a, ybuf_b, r1buf, r2buf, rbuf, yret_a, yret_b, tokb, t1buf, t2buf, zsend, zret, fin_src, fin_dst,
    pair_sem, z_s, z_r, ya_s, ya_r, yb_s, yb_r, x1_s, x1_r, x2_s, x2_r, b1_s, b1_r, b2_s, b2_r,
    w_l, w_s, w_r, g_s, g_r, h_s, h_r, r1_s, r1_r, r2_s, r2_r, t1_s, t1_r, t2_s, t2_r,
    yra_s, yra_r, yrb_s, yrb_r, zr_s, zr_r, fin_sem,
):
    me_e, me_s = lax.axis_index("expert"), lax.axis_index("shard")
    z_lo, y = me_e // 4, lax.rem(me_e, 4)
    z = (me_s // 8) * 2 + z_lo
    x = lax.rem(me_s // 2, 4)
    core = lax.rem(me_s, 2)
    sibling = device_of(x, y, z, 1 - core)
    left = device_of(lax.rem(x + 3, 4), y, z, core)
    right = device_of(lax.rem(x + 1, 4), y, z, core)

    def at_y(r):
        return device_of(x, lax.rem(y + r, 4), z, core)

    def at_z(d):
        return device_of(x, y, lax.rem(z + d, 8), core)

    barrier = pltpu.get_barrier_semaphore()
    greeted = [at_z(d) for d in (4, 3, 5, 2, 6, 1, 7)] + [at_y(r) for r in (2, 1, 3)] + [left, right, sibling]
    for device in greeted:
        pl.semaphore_signal(barrier, inc=1, device_id=device, device_id_type=MESH)

    own = 1
    TURNS = (0, 2, 4, 6)

    def turn(k):
        return 2 * k

    def place(d):
        return 2 * TURNS.index(d - 1) if d % 2 else 2 * TURNS.index((8 - d) % 8) + 1

    mine = pl.ds(pl.multiple_of(core * HALF, HALF), HALF)
    other = pl.ds(pl.multiple_of((1 - core) * HALF, HALF), HALF)
    local_weights = [
        pltpu.make_async_copy(wg_ref.at[0, mine], wgu.at[2], w_l.at[0]),
        pltpu.make_async_copy(wu_ref.at[0, mine], wgu.at[3], w_l.at[1]),
        pltpu.make_async_copy(wd_ref.at[0, :, mine], wdn.at[0], w_l.at[2]),
    ]
    pair_weights = [
        remote(wg_ref.at[0, other], wgu.at[0], w_s.at[0], w_r.at[0], sibling),
        remote(wu_ref.at[0, other], wgu.at[1], w_s.at[1], w_r.at[1], sibling),
        remote(wd_ref.at[0, :, other], wdn.at[1], w_s.at[2], w_r.at[2], sibling),
    ]
    for copy in local_weights:
        copy.start()

    tokens = tok_ref[...].astype(F32)
    scale = lax.rsqrt(jnp.mean(tokens * tokens, axis=-1, keepdims=True) + 1e-05)
    normed = tokens * scale * gain_ref[...]
    lanes = routing_lanes(columns_of(routes_ref[...]), columns_of(gates_ref[...]), cap_ref)
    first = core == 0
    own_half = jnp.where(first, normed[:, :HALF], normed[:, HALF:])
    pair_src[:, :HALF] = jnp.where(first, normed[:, HALF:], normed[:, :HALF]).astype(BF16)
    pair_src[:, HALF:] = lanes.astype(BF16)

    pl.semaphore_wait(barrier, len(greeted))
    pair = remote(pair_src, pair_dst, pair_sem.at[0], pair_sem.at[1], sibling)
    pair.start()
    for copy in pair_weights:
        copy.start()
    pair.wait_recv()
    their_half = pair_dst[:, :HALF].astype(F32)
    their_lanes = pair_dst[:, HALF:].astype(F32)
    ztok[own, :, :HALF] = jnp.concatenate(
        [jnp.where(first, own_half, their_half), jnp.where(first, their_half, own_half)], axis=0
    ).astype(BF16)
    ztok[own, :, HALF:] = jnp.concatenate(
        [jnp.where(first, lanes, their_lanes), jnp.where(first, their_lanes, lanes)], axis=0
    ).astype(BF16)

    def z_copy(d):
        n = place(d)
        return remote(ztok.at[own], ztok.at[n], z_s.at[n], z_r.at[n], at_z(8 - d))

    for d in (1, 3, 6, 5, 4, 7, 2):
        z_copy(d).start()

    def z_arrival(n):
        return remote(ztok.at[own], ztok.at[n], z_s.at[n], z_r.at[n], at_z(1))

    def weights_of(meta, turned):
        shape = (64, META) if turned else (META, 64)
        lane = lax.broadcasted_iota(jnp.int32, shape, 1 if turned else 0)
        column = lax.broadcasted_iota(jnp.int32, shape, 0 if turned else 1)
        expert = z_lo * 4 + (y + column // 16) % 4
        wanted = expert * 4 + column % 4
        pick = ((lane % 32 == wanted) & (lane < 96)).astype(F32).astype(BF16)
        if turned:
            raw = lax.dot_general(pick, meta, (((1,), (1,)), ((), ())), preferred_element_type=F32)
        else:
            raw = jnp.dot(meta, pick, preferred_element_type=F32)
        shape = (64, 32) if turned else (32, 64)
        column = lax.broadcasted_iota(jnp.int32, shape, 0 if turned else 1)
        row = lax.broadcasted_iota(jnp.int32, shape, 1 if turned else 0)
        return jnp.where(row // 8 == (column // 4) % 4, raw, 0.0)

    def picker_of(meta):
        return jnp.where(weights_of(meta, True) != 0.0, 1.0, 0.0).astype(BF16)

    def picked(picker, slab):
        return jnp.dot(picker, slab, preferred_element_type=F32).astype(BF16).reshape(4, 16, slab.shape[1])

    def combined(weights, rows):
        high = weights.astype(BF16)
        rest = (weights - high.astype(F32)).astype(BF16)
        made = jnp.dot(high, rows, preferred_element_type=F32) + jnp.dot(rest, rows, preferred_element_type=F32)
        return made.astype(BF16).reshape(2, 16, rows.shape[1])

    def ya_copy(k, r):
        return remote(sbuf_a.at[k, r - 1], xbuf_a.at[k, 0, 4 - r], ya_s.at[k, r - 1], ya_r.at[k, 3 - r], at_y(r))

    PARTS = ((0, 1), (1, 2), (3, 1))

    def yb_copy(k, part, r):
        rows = pl.ds(*PARTS[part])
        return remote(
            sbuf_b.at[k, r - 1, rows], xbuf_b.at[k, rows, 4 - r], yb_s.at[k, part, r - 1], yb_r.at[k, part, 3 - r], at_y(r)
        )

    def x1_copies(k):
        return (
            remote(xbuf_a.at[k, 0], xbuf_a.at[k, 1], x1_s.at[k, 0], x1_r.at[k, 0], right),
            remote(xbuf_a.at[k, 0], xbuf_a.at[k, 2], x1_s.at[k, 1], x1_r.at[k, 1], left),
        )

    def x2_copies(k):
        low, high = pl.ds(0, 2), pl.ds(2, 2)
        return (
            remote(xbuf_a.at[k, 1, low], xbuf_a.at[k, 3, low], x2_s.at[k, 0], x2_r.at[k, 0], right),
            remote(xbuf_a.at[k, 2, high], xbuf_a.at[k, 3, high], x2_s.at[k, 1], x2_r.at[k, 1], left),
        )

    def b1_copies(k):
        source = ztok.at[pl.ds(2 * k, 2), :, A:]
        return (
            remote(source, xtok.at[k, 0], b1_s.at[k, 0], b1_r.at[k, 0], right),
            remote(source, xtok.at[k, 1], b1_s.at[k, 1], b1_r.at[k, 1], left),
        )

    def b2_copies(k):
        return (
            remote(xtok.at[k, 0, 0], xtok.at[k, 2, 0], b2_s.at[k, 0], b2_r.at[k, 0], right),
            remote(xtok.at[k, 1, 1], xtok.at[k, 2, 1], b2_s.at[k, 1], b2_r.at[k, 1], left),
        )

    def dispatch(k):
        z_arrival(2 * k).wait_recv()

        @pl.when(k > 0)
        def _():
            z_arrival(2 * k + 1).wait_recv()

        for copy in b1_copies(k):
            copy.start()
        picker = picker_of(ztok[pl.ds(2 * k, 2), :, HALF:].reshape(32, META))

        def slots_at(start):
            return picked(picker, ztok[pl.ds(2 * k, 2), :, start : start + TILE].reshape(32, TILE))

        for start in range(0, A, TILE):
            slots = slots_at(start)
            xbuf_a[k, 0, 0, :, start : start + TILE] = slots[0]
            sbuf_a[k, :, :, start : start + TILE] = slots[1:]
        for r in (2, 1, 3):
            ya_copy(k, r).start()
        for start in range(0, B, TILE):
            slots = slots_at(A + start)
            xbuf_b[k, 0, 0, :, start : start + TILE] = slots[0]
            sbuf_b[k, :, 0, :, start : start + TILE] = slots[1:]
        for r in (2, 1, 3):
            yb_copy(k, 0, r).start()

    def dispatch_from(k, rel):
        picker = picker_of(xtok[k, rel - 1, :, :, B:].reshape(32, META))
        for start in range(0, B, TILE):
            slots = picked(picker, xtok[k, rel - 1, :, :, start : start + TILE].reshape(32, TILE))
            xbuf_b[k, rel, 0, :, start : start + TILE] = slots[0]
            sbuf_b[k, :, rel, :, start : start + TILE] = slots[1:]

    def gather_near(k):
        for near, far in zip(b1_copies(k), b2_copies(k)):
            near.wait_recv()
            far.start()
        for r in (1, 3, 2):
            ya_copy(k, r).wait_recv()
        for copy in x1_copies(k):
            copy.start()

        @pl.loop(1, 3)
        def _(rel):
            dispatch_from(k, rel)

        for r in (2, 1, 3):
            yb_copy(k, 1, r).start()

    def gather_far(k):
        for copy in b2_copies(k):
            copy.wait_recv()
        dispatch_from(k, 3)
        for r in (2, 1, 3):
            yb_copy(k, 2, r).start()
        for near, far in zip(x1_copies(k), x2_copies(k)):
            near.wait_recv()
            far.start()

    def pre_activations(k):
        return remote(gsend.at[k], grecv.at[k], g_s.at[k], g_r.at[k], sibling)

    def hidden_copy(k):
        return remote(hbuf.at[k, 0], hbuf.at[k, 1], h_s.at[k], h_r.at[k], sibling)

    def r1_copies(k):
        low, high = pl.ds(0, 2), pl.ds(2, 2)
        return (
            remote(ybuf_a.at[k, 3, low], r1buf.at[k, 0], r1_s.at[k, 0], r1_r.at[k, 0], left),
            remote(ybuf_a.at[k, 3, high], r1buf.at[k, 1], r1_s.at[k, 1], r1_r.at[k, 1], right),
        )

    def r2_copies(k):
        return (
            remote(ybuf_a.at[k, 1], r2buf.at[k, 1], r2_s.at[k, 1], r2_r.at[k, 1], left),
            remote(ybuf_a.at[k, 2], r2buf.at[k, 0], r2_s.at[k, 0], r2_r.at[k, 0], right),
        )

    def yra_copy(k, i):
        return remote(rbuf.at[k, i - 1], yret_a.at[k, 4 - i], yra_s.at[k, i - 1], yra_r.at[k, 3 - i], at_y(i))

    def yrb_copy(k, i):
        return remote(ybuf_b.at[k, :, i], yret_b.at[k, :, 3 - i], yrb_s.at[k, i - 1], yrb_r.at[k, 3 - i], at_y(i))

    def t1_copies(k):
        return (
            remote(tokb.at[k, 3, 0], t1buf.at[k, 0], t1_s.at[k, 0], t1_r.at[k, 0], left),
            remote(tokb.at[k, 3, 1], t1buf.at[k, 1], t1_s.at[k, 1], t1_r.at[k, 1], right),
        )

    def t2_copies(k):
        return (
            remote(tokb.at[k, 1], t2buf.at[k, 1], t2_s.at[k, 1], t2_r.at[k, 1], left),
            remote(tokb.at[k, 2], t2buf.at[k, 0], t2_s.at[k, 0], t2_r.at[k, 0], right),
        )

    def expert_hidden(k):
        @pl.when(k == 0)
        def _():
            for copy in local_weights:
                copy.wait()
            for copy in pair_weights:
                copy.wait_recv()

        for copy in x2_copies(k):
            copy.wait_recv()
        for part in range(3):
            for r in (1, 3, 2):
                yb_copy(k, part, r).wait_recv()

        def project(n):
            made = jnp.dot(xbuf_a[k].reshape(256, A), wgu[n, :A], preferred_element_type=F32)
            return made + jnp.dot(xbuf_b[k].reshape(256, B), wgu[n, A:], preferred_element_type=F32)

        @pl.loop(0, 2)
        def _(n):
            gsend[k, n] = project(n)

        pre_activations(k).start()

        @pl.loop(0, 2)
        def _(n):
            gown[n] = project(n + 2)

        pre_activations(k).wait_recv()
        gate = gown[0] + grecv[k, 0]
        up = gown[1] + grecv[k, 1]
        hbuf[k, 0] = (gate / (1.0 + jnp.exp(-gate)) * up).astype(BF16)
        hidden_copy(k).start()

    def expert_out(k):
        hidden_copy(k).wait_recv()

        def outputs(columns):
            made = jnp.dot(hbuf[k, 0], wdn[0, :, columns], preferred_element_type=F32)
            made = made + jnp.dot(hbuf[k, 1], wdn[1, :, columns], preferred_element_type=F32)
            return made.astype(BF16).reshape(4, 4, 16, TILE)

        for start in range(0, B, TILE):
            ybuf_b[k, :, :, :, start : start + TILE] = outputs(slice(A + start, A + start + TILE))

        for i in (2, 1, 3):
            yrb_copy(k, i).start()

        for start in range(0, A, TILE):
            ybuf_a[k, :, :, :, start : start + TILE] = outputs(slice(start, start + TILE))

        for copy in r1_copies(k):
            copy.start()

    def plus(ref, *others):
        total = ref[...].astype(F32)
        for term in others:
            total = total + term[...].astype(F32)
        return total.astype(BF16)

    def return_near(k):
        for copy in r1_copies(k):
            copy.wait_recv()
        ybuf_a[k, 1, 0:2] = plus(ybuf_a.at[k, 1, 0:2], r1buf.at[k, 0])
        ybuf_a[k, 2, 2:4] = plus(ybuf_a.at[k, 2, 2:4], r1buf.at[k, 1])
        for copy in r2_copies(k):
            copy.start()
        for i in (1, 3, 2):
            yrb_copy(k, i).wait_recv()

        def combine_for(rel, meta):
            weights = weights_of(meta.reshape(32, META), False)
            for start in range(0, B, TILE):
                columns = slice(start, start + TILE)
                rows = jnp.concatenate([ybuf_b[k, rel, 0, :, columns][None], yret_b[k, rel, :, :, columns]], axis=0)
                tokb[k, rel, :, :, columns] = combined(weights, rows.reshape(64, TILE))

        combine_for(3, xtok[k, 2, :, :, B:])
        for copy in t1_copies(k):
            copy.start()
        combine_for(0, ztok[pl.ds(2 * k, 2), :, HALF:])

        @pl.loop(1, 3)
        def _(rel):
            combine_for(rel, xtok[k, rel - 1, :, :, B:])

    def return_rows(k):
        for copy in t1_copies(k):
            copy.wait_recv()
        tokb[k, 1, 0] = plus(tokb.at[k, 1, 0], t1buf.at[k, 0])
        tokb[k, 2, 1] = plus(tokb.at[k, 2, 1], t1buf.at[k, 1])
        for copy in t2_copies(k):
            copy.start()
        for copy in r2_copies(k):
            copy.wait_recv()
        total = plus(ybuf_a.at[k, 0], r2buf.at[k, 0], r2buf.at[k, 1])
        yret_a[k, 0] = total[0]
        rbuf[k] = total[1:]
        for i in (2, 1, 3):
            yra_copy(k, i).start()

    def zr_copy(n, d):
        return remote(zsend.at[n], zret.at[n], zr_s.at[n], zr_r.at[n], at_z(d))

    def combine(k):
        for copy in t2_copies(k):
            copy.wait_recv()
        zsend[pl.ds(2 * k, 2), :, A:] = plus(tokb.at[k, 0], t2buf.at[k, 0], t2buf.at[k, 1])
        for r in (1, 3, 2):
            yra_copy(k, r).wait_recv()
        weights = weights_of(ztok[pl.ds(2 * k, 2), :, HALF:].reshape(32, META), False)
        for start in range(0, A, TILE):
            columns = slice(start, start + TILE)
            zsend[pl.ds(2 * k, 2), :, columns] = combined(weights, yret_a[k, :, :, columns].reshape(64, TILE))
        zr_copy(2 * k, turn(k) + 1).start()

        @pl.when(k > 0)
        def _():
            zr_copy(2 * k + 1, 8 - turn(k)).start()

    def when(k, work):
        @pl.when((k >= 0) & (k < CHUNKS))
        def _():
            work(k)

    dispatch(0)

    def step_of(t, carry):
        when(t - 1, gather_far)
        when(t + 0, gather_near)
        when(t + 1, dispatch)
        when(t - 2, expert_hidden)
        when(t - 3, return_near)
        when(t - 2, expert_out)
        when(t - 4, return_rows)
        when(t - 5, combine)
        return carry

    lax.fori_loop(0, CHUNKS + 5, step_of, 0)

    total = zsend[own].astype(F32)
    for n in (0, 2, 3, 4, 5, 6, 7):
        zr_copy(n, 1).wait_recv()
        total = total + zret[n].astype(F32)
    total = total.astype(BF16).astype(F32)
    fin_src[...] = jnp.where(first, total[8:], total[:8]).astype(BF16)
    fin = remote(fin_src, fin_dst, fin_sem.at[0], fin_sem.at[1], sibling)
    fin.start()
    kept = jnp.where(first, total[:8], total[8:])
    fin.wait_recv()
    theirs = fin_dst[...].astype(F32)
    out_ref[:, :HALF] = jnp.where(first, kept, theirs).astype(BF16)
    out_ref[:, HALF:] = jnp.where(first, theirs, kept).astype(BF16)

    fin.wait_send()
    pair.wait_send()
    for copy in pair_weights:
        copy.wait_send()
    for d in range(1, 8):
        z_copy(d).wait_send()
    for n in (0, 2, 3, 4, 5, 6, 7):
        zr_copy(n, 1).wait_send()

    def sent(k, carry):
        for r in (1, 2, 3):
            ya_copy(k, r).wait_send()
            yra_copy(k, r).wait_send()
            yrb_copy(k, r).wait_send()
            for part in range(3):
                yb_copy(k, part, r).wait_send()
        for copies in (x1_copies, x2_copies, b1_copies, b2_copies, r1_copies, r2_copies, t1_copies, t2_copies):
            for copy in copies(k):
                copy.wait_send()
        pre_activations(k).wait_send()
        hidden_copy(k).wait_send()
        return carry

    lax.fori_loop(0, CHUNKS, sent, 0)


def on_device(tokens, norm_gain, routes, gate_weights, capacity, w_gate, w_up, w_down):
    vmem, smem = pl.BlockSpec(memory_space=pltpu.VMEM), pl.BlockSpec(memory_space=pltpu.SMEM)
    whole = pl.BlockSpec(memory_space=pl.ANY)
    k = CHUNKS

    def held(*shape, dtype=BF16):
        return pltpu.VMEM(shape, dtype)

    def sems(*shape):
        return [pltpu.SemaphoreType.DMA(shape)]

    return pl.pallas_call(
        kernel,
        out_shape=jax.ShapeDtypeStruct((8, D), BF16),
        in_specs=[vmem, vmem, vmem, vmem, smem, whole, whole, whole],
        out_specs=vmem,
        scratch_shapes=[
            held(8, HALF + META),
            held(8, HALF + META),
            held(8, 16, HALF + META),
            held(k, 3, 16, A),
            held(k, 3, 4, 16, B),
            held(k, 3, 2, 16, B + META),
            held(k, 4, 4, 16, A),
            held(k, 4, 4, 16, B),
            held(4, HALF, FW),
            held(2, FW, HALF),
            held(k, 2, 256, FW, dtype=F32),
            held(k, 2, 256, FW, dtype=F32),
            held(2, 256, FW, dtype=F32),
            held(k, 2, 256, FW),
            held(k, 4, 4, 16, A),
            held(k, 4, 4, 16, B),
            held(k, 2, 2, 16, A),
            held(k, 2, 4, 16, A),
            held(k, 3, 16, A),
            held(k, 4, 16, A),
            held(k, 4, 3, 16, B),
            held(k, 4, 2, 16, B),
            held(k, 2, 16, B),
            held(k, 2, 2, 16, B),
            held(8, 16, HALF),
            held(8, 16, HALF),
            held(8, HALF),
            held(8, HALF),
        ]
        + sems(2)
        + sems(8) * 2
        + sems(k, 3) * 2
        + sems(k, 3, 3) * 2
        + sems(k, 2) * 8
        + sems(3) * 3
        + sems(k) * 4
        + sems(k, 2) * 8
        + sems(k, 3) * 4
        + sems(8) * 2
        + sems(2),
        compiler_params=pltpu.CompilerParams(
            collective_id=0, has_side_effects=True, vmem_limit_bytes=67043328
        ),
    )(tokens, norm_gain[None], routes.T, gate_weights.T, capacity, w_gate, w_up, w_down)


def solution(mesh):
    in_specs = (
        P(("expert", "shard"), None),
        P(),
        P(("expert", "shard"), None),
        P(("expert", "shard"), None),
        P(),
        P("expert", None, "shard"),
        P("expert", None, "shard"),
        P("expert", "shard", None),
    )
    out_specs = P(("expert", "shard"), None)
    return jax.shard_map(
        on_device, mesh=mesh, in_specs=in_specs, out_specs=out_specs, check_vma=False
    )
```

```python
import jax
import jax.numpy as jnp
from jax import lax
from jax.experimental import pallas as pl
from jax.experimental.pallas import tpu as pltpu
from jax.sharding import PartitionSpec as P

MESH = pl.DeviceIdType.MESH
F32, BF16 = jnp.float32, jnp.bfloat16

D = 6144
HALF = D // 2
FW = 256
META = 128
CHUNKS = 4
A = 1664
B = HALF - A
TILE = 256
LOW, HIGH = pl.ds(0, 2), pl.ds(2, 2)
ORDER = (
    "d0", "nb0", "nd0", "na0", "d1", "fb0", "fa0", "nb1", "d2", "d3", "nb2", "nd2", "na1", "na2", "fb2", "fb1",
    "nb3", "nd1", "fa2", "nd3", "fa1", "na3", "h2", "fb3", "fa3", "o2", "h1", "Na2", "o1", "Nc2", "Nb2", "h3", "Ra2",
    "Na1", "Rb2", "o3", "Nc1", "h0", "Nc3", "Na3", "Ra1", "C2", "Nb1", "Rb1", "o0", "Na0", "C1", "Nb3", "Nc0", "Ra3",
    "Rb3", "Nb0", "Ra0", "Rb0", "C3", "C0",
)
FIRST = 2


def tiles_of(width):
    return [(start, min(TILE, width - start)) for start in range(0, width, TILE)]


def device_of(x, y, z, core):
    return (lax.rem(z, 2) * 4 + y, (z // 2) * 8 + x * 2 + core)


def remote(src, dst, send, recv, device):
    return pltpu.make_async_remote_copy(
        src_ref=src,
        dst_ref=dst,
        send_sem=send,
        recv_sem=recv,
        device_id=device,
        device_id_type=MESH,
    )


def columns_of(pair):
    row = lax.broadcasted_iota(jnp.int32, (8, 8), 0)
    lane = lax.broadcasted_iota(jnp.int32, (8, 8), 1)
    spread = [jnp.broadcast_to(pair[k : k + 1, :], (8, 8)) for k in range(2)]
    zero = jnp.zeros((8, 8), pair.dtype)
    return [jnp.sum(jnp.where(row == lane, s, zero), axis=1, keepdims=True) for s in spread]


def routing_lanes(routes, gates, cap_ref):
    lane = lax.broadcasted_iota(jnp.int32, (8, META), 1)
    row = lax.broadcasted_iota(jnp.int32, (8, META), 0)
    expert, slot = lane // 4, lane % 4
    named = [routes[k] == expert for k in range(2)]
    either = (named[0] | named[1]).astype(jnp.int32)
    running = either
    for shift in (1, 2, 4):
        running = running + jnp.where(row >= shift, pltpu.roll(running, shift, 0), 0)
    rank = running - either
    limit = jnp.zeros((8, META), jnp.int32)
    for e in range(8):
        limit = jnp.where(expert == e, cap_ref[e], limit)
    held = (rank == slot) & (rank < limit)
    weights = jnp.zeros((8, META), F32)
    for k in range(2):
        weights = weights + jnp.where(named[k] & held, gates[k], 0.0)
    high = weights.astype(BF16).astype(F32)
    middle = (weights - high).astype(BF16).astype(F32)
    low = weights - high - middle
    return high + pltpu.roll(middle, 32, 1) + pltpu.roll(low, 64, 1)


def kernel(
    tok_ref, gain_ref, routes_ref, gates_ref, cap_ref, wg_ref, wu_ref, wd_ref, out_ref,
    pair_src, pair_dst, ztok, sbuf_a, sbuf_b, xtok, xbuf_a, xbuf_b, wgu, wdn, gsend, grecv, gown, hbuf,
    ybuf_a, ybuf_b, r1buf, r2buf, rbuf, yret_a, yret_b, tokb, t1buf, t2buf, zsend, zret, fin_src, fin_dst,
    pair_sem, z_s, z_r, ya_s, ya_r, yb_s, yb_r, x1_s, x1_r, x2_s, x2_r, b1_s, b1_r, b2_s, b2_r,
    w_l, w_s, w_r, g_s, g_r, h_s, h_r, r1_s, r1_r, r2_s, r2_r, t1_s, t1_r, t2_s, t2_r,
    yra_s, yra_r, yrb_s, yrb_r, zr_s, zr_r, fin_sem,
):
    me_e, me_s = lax.axis_index("expert"), lax.axis_index("shard")
    z_lo, y = me_e // 4, lax.rem(me_e, 4)
    z = (me_s // 8) * 2 + z_lo
    x = lax.rem(me_s // 2, 4)
    core = lax.rem(me_s, 2)
    sibling = device_of(x, y, z, 1 - core)
    left = device_of(lax.rem(x + 3, 4), y, z, core)
    right = device_of(lax.rem(x + 1, 4), y, z, core)

    def at_y(r):
        return device_of(x, lax.rem(y + r, 4), z, core)

    def at_z(d):
        return device_of(x, y, lax.rem(z + d, 8), core)

    barrier = pltpu.get_barrier_semaphore()
    greeted = [at_z(d) for d in (4, 3, 5, 2, 6, 1, 7)] + [at_y(r) for r in (2, 1, 3)] + [left, right, sibling]
    for device in greeted:
        pl.semaphore_signal(barrier, inc=1, device_id=device, device_id_type=MESH)

    own = 1
    TURNS = (0, 2, 4, 6)

    def place(d):
        return 2 * TURNS.index(d - 1) if d % 2 else 2 * TURNS.index((8 - d) % 8) + 1

    mine = pl.ds(pl.multiple_of(core * HALF, HALF), HALF)
    other = pl.ds(pl.multiple_of((1 - core) * HALF, HALF), HALF)
    local_weights = [
        pltpu.make_async_copy(wg_ref.at[0, mine], wgu.at[2], w_l.at[0]),
        pltpu.make_async_copy(wu_ref.at[0, mine], wgu.at[3], w_l.at[1]),
        pltpu.make_async_copy(wd_ref.at[0, :, mine], wdn.at[0], w_l.at[2]),
    ]
    pair_weights = [
        remote(wg_ref.at[0, other], wgu.at[0], w_s.at[0], w_r.at[0], sibling),
        remote(wu_ref.at[0, other], wgu.at[1], w_s.at[1], w_r.at[1], sibling),
        remote(wd_ref.at[0, :, other], wdn.at[1], w_s.at[2], w_r.at[2], sibling),
    ]
    for copy in local_weights:
        copy.start()

    tokens = tok_ref[...].astype(F32)
    scale = lax.rsqrt(jnp.mean(tokens * tokens, axis=-1, keepdims=True) + 1e-05)
    normed = tokens * scale * gain_ref[...]
    lanes = routing_lanes(columns_of(routes_ref[...]), columns_of(gates_ref[...]), cap_ref)
    first = core == 0
    own_half = jnp.where(first, normed[:, :HALF], normed[:, HALF:])
    pair_src[:, :HALF] = jnp.where(first, normed[:, HALF:], normed[:, :HALF]).astype(BF16)
    pair_src[:, HALF:] = lanes.astype(BF16)

    pl.semaphore_wait(barrier, len(greeted))
    pair = remote(pair_src, pair_dst, pair_sem.at[0], pair_sem.at[1], sibling)
    pair.start()
    for copy in pair_weights:
        copy.start()
    pair.wait_recv()
    their_half = pair_dst[:, :HALF].astype(F32)
    their_lanes = pair_dst[:, HALF:].astype(F32)
    ztok[own, :, :HALF] = jnp.concatenate(
        [jnp.where(first, own_half, their_half), jnp.where(first, their_half, own_half)], axis=0
    ).astype(BF16)
    ztok[own, :, HALF:] = jnp.concatenate(
        [jnp.where(first, lanes, their_lanes), jnp.where(first, their_lanes, lanes)], axis=0
    ).astype(BF16)

    def z_copy(d):
        n = place(d)
        return remote(ztok.at[own], ztok.at[n], z_s.at[n], z_r.at[n], at_z(8 - d))

    for d in (1, 3, 6, 5, 4, 7, 2):
        z_copy(d).start()

    def z_arrival(n):
        return remote(ztok.at[own], ztok.at[n], z_s.at[n], z_r.at[n], at_z(1))

    def weights_of(meta, turned):
        shape = (64, META) if turned else (META, 64)
        lane = lax.broadcasted_iota(jnp.int32, shape, 1 if turned else 0)
        column = lax.broadcasted_iota(jnp.int32, shape, 0 if turned else 1)
        expert = z_lo * 4 + (y + column // 16) % 4
        wanted = expert * 4 + column % 4
        pick = ((lane % 32 == wanted) & (lane < 96)).astype(F32).astype(BF16)
        if turned:
            raw = lax.dot_general(pick, meta, (((1,), (1,)), ((), ())), preferred_element_type=F32)
        else:
            raw = jnp.dot(meta, pick, preferred_element_type=F32)
        shape = (64, 32) if turned else (32, 64)
        column = lax.broadcasted_iota(jnp.int32, shape, 0 if turned else 1)
        row = lax.broadcasted_iota(jnp.int32, shape, 1 if turned else 0)
        return jnp.where(row // 8 == (column // 4) % 4, raw, 0.0)

    def picker_of(meta):
        return jnp.where(weights_of(meta, True) != 0.0, 1.0, 0.0).astype(BF16)

    def picked(picker, slab):
        return jnp.dot(picker, slab, preferred_element_type=F32).astype(BF16).reshape(4, 16, slab.shape[1])

    def combined(weights, rows):
        high = weights.astype(BF16)
        rest = (weights - high.astype(F32)).astype(BF16)
        made = jnp.dot(high, rows, preferred_element_type=F32) + jnp.dot(rest, rows, preferred_element_type=F32)
        return made.astype(BF16).reshape(2, 16, rows.shape[1])

    def ya_copy(k, r):
        return remote(sbuf_a.at[k, r - 1], xbuf_a.at[k, 0, 4 - r], ya_s.at[k, r - 1], ya_r.at[k, 3 - r], at_y(r))

    PARTS = ((0, 1), (1, 2), (3, 1))

    def yb_copy(k, part, r):
        rows = pl.ds(*PARTS[part])
        return remote(
            sbuf_b.at[k, r - 1, rows], xbuf_b.at[k, rows, 4 - r], yb_s.at[k, part, r - 1], yb_r.at[k, part, 3 - r], at_y(r)
        )

    def x1_copies(k):
        def copy(way, turn, rows, device):
            return remote(
                xbuf_a.at[k, 0, rows], xbuf_a.at[k, 1 + way, rows], x1_s.at[k, way, turn], x1_r.at[k, way, turn], device
            )

        return copy(0, 0, LOW, right), copy(1, 0, HIGH, left), copy(0, 1, HIGH, right), copy(1, 1, LOW, left)

    def x2_copies(k):
        return (
            remote(xbuf_a.at[k, 1, LOW], xbuf_a.at[k, 3, LOW], x2_s.at[k, 0], x2_r.at[k, 0], right),
            remote(xbuf_a.at[k, 2, HIGH], xbuf_a.at[k, 3, HIGH], x2_s.at[k, 1], x2_r.at[k, 1], left),
        )

    def b1_copies(k):
        def copy(way, turn, n, device):
            return remote(
                ztok.at[2 * k + n, :, A:], xtok.at[k, way, n], b1_s.at[k, way, turn], b1_r.at[k, way, turn], device
            )

        return copy(0, 0, 0, right), copy(1, 0, 1, left), copy(0, 1, 1, right), copy(1, 1, 0, left)

    def b2_copies(k):
        return (
            remote(xtok.at[k, 0, 0], xtok.at[k, 2, 0], b2_s.at[k, 0], b2_r.at[k, 0], right),
            remote(xtok.at[k, 1, 1], xtok.at[k, 2, 1], b2_s.at[k, 1], b2_r.at[k, 1], left),
        )

    def dispatch(k):
        z_arrival(2 * k).wait_recv()

        if k > 0:
            z_arrival(2 * k + 1).wait_recv()
        for copy in b1_copies(k):
            copy.start()
        picker = picker_of(ztok[pl.ds(2 * k, 2), :, HALF:].reshape(32, META))

        def slots_at(start, width):
            return picked(picker, ztok[pl.ds(2 * k, 2), :, start : start + width].reshape(32, width))

        for start, width in tiles_of(A):
            slots = slots_at(start, width)
            xbuf_a[k, 0, 0, :, start : start + width] = slots[0]
            sbuf_a[k, :, :, start : start + width] = slots[1:]
        for r in (2, 1, 3):
            ya_copy(k, r).start()
        for start, width in tiles_of(B):
            slots = slots_at(A + start, width)
            xbuf_b[k, 0, 0, :, start : start + width] = slots[0]
            sbuf_b[k, :, 0, :, start : start + width] = slots[1:]
        for r in (2, 1, 3):
            yb_copy(k, 0, r).start()

    def dispatch_from(k, rel):
        picker = picker_of(xtok[k, rel - 1, :, :, B:].reshape(32, META))
        for start, width in tiles_of(B):
            slots = picked(picker, xtok[k, rel - 1, :, :, start : start + width].reshape(32, width))
            xbuf_b[k, rel, 0, :, start : start + width] = slots[0]
            sbuf_b[k, :, rel, :, start : start + width] = slots[1:]

    def pass_tokens(k):
        for near, far in zip(b1_copies(k), b2_copies(k)):
            near.wait_recv()
            far.start()

    def ring_slots(k):
        for r in (1, 3, 2):
            ya_copy(k, r).wait_recv()
        for copy in x1_copies(k):
            copy.start()

    def dispatch_near(k):
        for copy in b1_copies(k)[2:]:
            copy.wait_recv()

        @pl.loop(1, 3)
        def _(rel):
            dispatch_from(k, rel)

        for r in (2, 1, 3):
            yb_copy(k, 1, r).start()

    def dispatch_far(k):
        for copy in b2_copies(k):
            copy.wait_recv()
        dispatch_from(k, 3)
        for r in (2, 1, 3):
            yb_copy(k, 2, r).start()

    def pass_slots(k):
        for near, far in zip(x1_copies(k), x2_copies(k)):
            near.wait_recv()
            far.start()

    def pre_activations(k):
        return remote(gsend.at[k], grecv.at[k], g_s.at[k], g_r.at[k], sibling)

    def hidden_copy(k):
        return remote(hbuf.at[k, 0], hbuf.at[k, 1], h_s.at[k], h_r.at[k], sibling)

    def r1_copies(k):
        return (
            remote(ybuf_a.at[k, 3, LOW], r1buf.at[k, 0], r1_s.at[k, 0], r1_r.at[k, 0], left),
            remote(ybuf_a.at[k, 3, HIGH], r1buf.at[k, 1], r1_s.at[k, 1], r1_r.at[k, 1], right),
        )

    def r2_copies(k):
        def copy(way, turn, rows, device):
            return remote(
                ybuf_a.at[k, 1 + way, rows], r2buf.at[k, 1 - way, rows], r2_s.at[k, way, turn], r2_r.at[k, way, turn], device
            )

        return copy(0, 0, HIGH, left), copy(1, 0, LOW, right), copy(0, 1, LOW, left), copy(1, 1, HIGH, right)

    def yra_copy(k, i):
        return remote(rbuf.at[k, i - 1], yret_a.at[k, 4 - i], yra_s.at[k, i - 1], yra_r.at[k, 3 - i], at_y(i))

    RETURNS = ((3, 1), (0, 3))

    def yrb_copy(k, part, i):
        rows = pl.ds(*RETURNS[part])
        return remote(
            ybuf_b.at[k, rows, i], yret_b.at[k, rows, 3 - i], yrb_s.at[k, part, i - 1], yrb_r.at[k, part, 3 - i], at_y(i)
        )

    def t1_copies(k):
        return (
            remote(tokb.at[k, 3, 0], t1buf.at[k, 0], t1_s.at[k, 0], t1_r.at[k, 0], left),
            remote(tokb.at[k, 3, 1], t1buf.at[k, 1], t1_s.at[k, 1], t1_r.at[k, 1], right),
        )

    def t2_copies(k):
        def copy(way, turn, n, device):
            return remote(
                tokb.at[k, 1 + way, n], t2buf.at[k, 1 - way, n], t2_s.at[k, way, turn], t2_r.at[k, way, turn], device
            )

        return copy(0, 0, 1, left), copy(1, 0, 0, right), copy(0, 1, 0, left), copy(1, 1, 1, right)

    def expert_hidden(k):
        if k == FIRST:
            for copy in local_weights:
                copy.wait()
            for copy in pair_weights:
                copy.wait_recv()
        for copy in x1_copies(k)[2:] + x2_copies(k):
            copy.wait_recv()
        for part in range(3):
            for r in (1, 3, 2):
                yb_copy(k, part, r).wait_recv()

        def project(n):
            made = jnp.dot(xbuf_a[k].reshape(256, A), wgu[n, :A], preferred_element_type=F32)
            return made + jnp.dot(xbuf_b[k].reshape(256, B), wgu[n, A:], preferred_element_type=F32)

        @pl.loop(0, 2)
        def _(n):
            gsend[k, n] = project(n)

        pre_activations(k).start()

        @pl.loop(0, 2)
        def _(n):
            gown[n] = project(n + 2)

        pre_activations(k).wait_recv()
        gate = gown[0] + grecv[k, 0]
        up = gown[1] + grecv[k, 1]
        hbuf[k, 0] = (gate / (1.0 + jnp.exp(-gate)) * up).astype(BF16)
        hidden_copy(k).start()

    def expert_out(k):
        hidden_copy(k).wait_recv()

        def outputs(start, width):
            columns = slice(start, start + width)
            made = jnp.dot(hbuf[k, 0], wdn[0, :, columns], preferred_element_type=F32)
            made = made + jnp.dot(hbuf[k, 1], wdn[1, :, columns], preferred_element_type=F32)
            return made.astype(BF16).reshape(4, 4, 16, width)

        for start, width in tiles_of(B):
            ybuf_b[k, :, :, :, start : start + width] = outputs(A + start, width)
        for part in range(2):
            for i in (2, 1, 3):
                yrb_copy(k, part, i).start()
        for start, width in tiles_of(A):
            ybuf_a[k, :, :, :, start : start + width] = outputs(start, width)
        for copy in r1_copies(k) + r2_copies(k)[:2]:
            copy.start()

    def plus(ref, *others):
        total = ref[...].astype(F32)
        for term in others:
            total = total + term[...].astype(F32)
        return total.astype(BF16)

    def sum_slots(k):
        for copy in r1_copies(k):
            copy.wait_recv()
        ybuf_a[k, 1, 0:2] = plus(ybuf_a.at[k, 1, 0:2], r1buf.at[k, 0])
        ybuf_a[k, 2, 2:4] = plus(ybuf_a.at[k, 2, 2:4], r1buf.at[k, 1])
        for copy in r2_copies(k)[2:]:
            copy.start()

    def combine_for(k, rel, meta):
        weights = weights_of(meta.reshape(32, META), False)
        for start, width in tiles_of(B):
            columns = slice(start, start + width)
            rows = jnp.concatenate([ybuf_b[k, rel, 0, :, columns][None], yret_b[k, rel, :, :, columns]], axis=0)
            tokb[k, rel, :, :, columns] = combined(weights, rows.reshape(64, width))

    def combine_far(k):
        for i in (1, 3, 2):
            yrb_copy(k, 0, i).wait_recv()
        combine_for(k, 3, xtok[k, 2, :, :, B:])
        for copy in t1_copies(k):
            copy.start()

    def combine_near(k):
        for i in (1, 3, 2):
            yrb_copy(k, 1, i).wait_recv()

        @pl.loop(1, 3)
        def _(rel):
            combine_for(k, rel, xtok[k, rel - 1, :, :, B:])

        for copy in t2_copies(k)[:2]:
            copy.start()
        combine_for(k, 0, ztok[pl.ds(2 * k, 2), :, HALF:])

    def sum_tokens(k):
        for copy in t1_copies(k):
            copy.wait_recv()
        tokb[k, 1, 0] = plus(tokb.at[k, 1, 0], t1buf.at[k, 0])
        tokb[k, 2, 1] = plus(tokb.at[k, 2, 1], t1buf.at[k, 1])
        for copy in t2_copies(k)[2:]:
            copy.start()

    def return_slots(k):
        for copy in r2_copies(k):
            copy.wait_recv()
        total = plus(ybuf_a.at[k, 0], r2buf.at[k, 0], r2buf.at[k, 1])
        yret_a[k, 0] = total[0]
        rbuf[k] = total[1:]
        for i in (2, 1, 3):
            yra_copy(k, i).start()

    def zr_copy(n, d):
        return remote(zsend.at[n], zret.at[n], zr_s.at[n], zr_r.at[n], at_z(d))

    def combine(k):
        for copy in t2_copies(k):
            copy.wait_recv()
        zsend[pl.ds(2 * k, 2), :, A:] = plus(tokb.at[k, 0], t2buf.at[k, 0], t2buf.at[k, 1])
        for r in (1, 3, 2):
            yra_copy(k, r).wait_recv()
        weights = weights_of(ztok[pl.ds(2 * k, 2), :, HALF:].reshape(32, META), False)
        for start, width in tiles_of(A):
            columns = slice(start, start + width)
            zsend[pl.ds(2 * k, 2), :, columns] = combined(weights, yret_a[k, :, :, columns].reshape(64, width))
        zr_copy(2 * k, TURNS[k] + 1).start()
        if k > 0:
            zr_copy(2 * k + 1, 8 - TURNS[k]).start()

    stages = {
        "d": dispatch,
        "nb": pass_tokens,
        "na": ring_slots,
        "nd": dispatch_near,
        "fb": dispatch_far,
        "fa": pass_slots,
        "h": expert_hidden,
        "o": expert_out,
        "Na": sum_slots,
        "Nc": combine_far,
        "Nb": combine_near,
        "Rb": sum_tokens,
        "Ra": return_slots,
        "C": combine,
    }
    for name in ORDER:
        stages[name[:-1]](int(name[-1]))

    total = zsend[own].astype(F32)
    for n in (0, 2, 3, 4, 5, 6, 7):
        zr_copy(n, 1).wait_recv()
        total = total + zret[n].astype(F32)
    total = total.astype(BF16).astype(F32)
    fin_src[...] = jnp.where(first, total[8:], total[:8]).astype(BF16)
    fin = remote(fin_src, fin_dst, fin_sem.at[0], fin_sem.at[1], sibling)
    fin.start()
    kept = jnp.where(first, total[:8], total[8:])
    fin.wait_recv()
    theirs = fin_dst[...].astype(F32)
    out_ref[:, :HALF] = jnp.where(first, kept, theirs).astype(BF16)
    out_ref[:, HALF:] = jnp.where(first, theirs, kept).astype(BF16)

    fin.wait_send()
    pair.wait_send()
    for copy in pair_weights:
        copy.wait_send()
    for d in range(1, 8):
        z_copy(d).wait_send()
    for n in (0, 2, 3, 4, 5, 6, 7):
        zr_copy(n, 1).wait_send()

    def sent(k, carry):
        for r in (1, 2, 3):
            ya_copy(k, r).wait_send()
            yra_copy(k, r).wait_send()
            for part in range(2):
                yrb_copy(k, part, r).wait_send()
            for part in range(3):
                yb_copy(k, part, r).wait_send()
        for copies in (x1_copies, x2_copies, b1_copies, b2_copies, r1_copies, r2_copies, t1_copies, t2_copies):
            for copy in copies(k):
                copy.wait_send()
        pre_activations(k).wait_send()
        hidden_copy(k).wait_send()
        return carry

    lax.fori_loop(0, CHUNKS, sent, 0)


def on_device(tokens, norm_gain, routes, gate_weights, capacity, w_gate, w_up, w_down):
    vmem, smem = pl.BlockSpec(memory_space=pltpu.VMEM), pl.BlockSpec(memory_space=pltpu.SMEM)
    whole = pl.BlockSpec(memory_space=pl.ANY)
    k = CHUNKS

    def held(*shape, dtype=BF16):
        return pltpu.VMEM(shape, dtype)

    def sems(*shape):
        return [pltpu.SemaphoreType.DMA(shape)]

    return pl.pallas_call(
        kernel,
        out_shape=jax.ShapeDtypeStruct((8, D), BF16),
        in_specs=[vmem, vmem, vmem, vmem, smem, whole, whole, whole],
        out_specs=vmem,
        scratch_shapes=[
            held(8, HALF + META),
            held(8, HALF + META),
            held(8, 16, HALF + META),
            held(k, 3, 16, A),
            held(k, 3, 4, 16, B),
            held(k, 3, 2, 16, B + META),
            held(k, 4, 4, 16, A),
            held(k, 4, 4, 16, B),
            held(4, HALF, FW),
            held(2, FW, HALF),
            held(k, 2, 256, FW, dtype=F32),
            held(k, 2, 256, FW, dtype=F32),
            held(2, 256, FW, dtype=F32),
            held(k, 2, 256, FW),
            held(k, 4, 4, 16, A),
            held(k, 4, 4, 16, B),
            held(k, 2, 2, 16, A),
            held(k, 2, 4, 16, A),
            held(k, 3, 16, A),
            held(k, 4, 16, A),
            held(k, 4, 3, 16, B),
            held(k, 4, 2, 16, B),
            held(k, 2, 16, B),
            held(k, 2, 2, 16, B),
            held(8, 16, HALF),
            held(8, 16, HALF),
            held(8, HALF),
            held(8, HALF),
        ]
        + sems(2)
        + sems(8) * 2
        + sems(k, 3) * 2
        + sems(k, 3, 3) * 2
        + (sems(k, 2, 2) * 2 + sems(k, 2) * 2) * 2
        + sems(3) * 3
        + sems(k) * 4
        + (sems(k, 2) * 2 + sems(k, 2, 2) * 2) * 2
        + sems(k, 3) * 2
        + sems(k, 2, 3) * 2
        + sems(8) * 2
        + sems(2),
        compiler_params=pltpu.CompilerParams(
            collective_id=0, has_side_effects=True, vmem_limit_bytes=67043328
        ),
    )(tokens, norm_gain[None], routes.T, gate_weights.T, capacity, w_gate, w_up, w_down)


def solution(mesh):
    in_specs = (
        P(("expert", "shard"), None),
        P(),
        P(("expert", "shard"), None),
        P(("expert", "shard"), None),
        P(),
        P("expert", None, "shard"),
        P("expert", None, "shard"),
        P("expert", "shard", None),
    )
    out_specs = P(("expert", "shard"), None)
    return jax.shard_map(
        on_device, mesh=mesh, in_specs=in_specs, out_specs=out_specs, check_vma=False
    )
```

```python
import jax
import jax.numpy as jnp
from jax import lax
from jax.experimental import pallas as pl
from jax.experimental.pallas import tpu as pltpu
from jax.sharding import PartitionSpec as P

MESH = pl.DeviceIdType.MESH
F32, BF16 = jnp.float32, jnp.bfloat16

D = 6144
HALF = D // 2
FW = 256
META = 128
CHUNKS = 4
A = 1664
B = HALF - A
TILE = 256
LOW, HIGH = pl.ds(0, 2), pl.ds(2, 2)
ORDER = (
    "d0", "nb0", "nd0", "na0", "d1", "fb0", "fa0", "nb1", "d2", "d3", "nb2", "nd2", "na1", "na2", "fb2", "fb1",
    "nb3", "nd1", "fa2", "nd3", "fa1", "na3", "h2", "fb3", "fa3", "o2", "h1", "Na2", "o1", "Nc2", "Nb2", "h3", "Ra2",
    "Na1", "Rb2", "o3", "Nc1", "h0", "Nc3", "Na3", "Ra1", "C2", "Nb1", "Rb1", "o0", "Na0", "C1", "Nb3", "Nc0", "Ra3",
    "Rb3", "Nb0", "Ra0", "Rb0", "C3", "C0",
)
FIRST = 2


def tiles_of(width):
    return [(start, min(TILE, width - start)) for start in range(0, width, TILE)]


def device_of(x, y, z, core):
    return (lax.rem(z, 2) * 4 + y, (z // 2) * 8 + x * 2 + core)


def remote(src, dst, send, recv, device):
    return pltpu.make_async_remote_copy(
        src_ref=src,
        dst_ref=dst,
        send_sem=send,
        recv_sem=recv,
        device_id=device,
        device_id_type=MESH,
    )


def columns_of(pair):
    row = lax.broadcasted_iota(jnp.int32, (8, 8), 0)
    lane = lax.broadcasted_iota(jnp.int32, (8, 8), 1)
    spread = [jnp.broadcast_to(pair[k : k + 1, :], (8, 8)) for k in range(2)]
    zero = jnp.zeros((8, 8), pair.dtype)
    return [jnp.sum(jnp.where(row == lane, s, zero), axis=1, keepdims=True) for s in spread]


def routing_lanes(routes, gates, cap_ref):
    lane = lax.broadcasted_iota(jnp.int32, (8, META), 1)
    row = lax.broadcasted_iota(jnp.int32, (8, META), 0)
    expert, slot = lane // 4, lane % 4
    named = [routes[k] == expert for k in range(2)]
    either = (named[0] | named[1]).astype(jnp.int32)
    running = either
    for shift in (1, 2, 4):
        running = running + jnp.where(row >= shift, pltpu.roll(running, shift, 0), 0)
    rank = running - either
    limit = jnp.zeros((8, META), jnp.int32)
    for e in range(8):
        limit = jnp.where(expert == e, cap_ref[e], limit)
    held = (rank == slot) & (rank < limit)
    weights = jnp.zeros((8, META), F32)
    for k in range(2):
        weights = weights + jnp.where(named[k] & held, gates[k], 0.0)
    high = weights.astype(BF16).astype(F32)
    middle = (weights - high).astype(BF16).astype(F32)
    low = weights - high - middle
    return high + pltpu.roll(middle, 32, 1) + pltpu.roll(low, 64, 1)


def kernel(
    tok_hbm, gain_hbm, routes_hbm, gates_hbm, cap_hbm, wg_ref, wu_ref, wd_ref, out_ref,
    tok_ref, gain_ref, routes_ref, gates_ref, cap_ref,
    pair_src, pair_dst, ztok, sbuf_a, sbuf_b, xtok, xbuf_a, xbuf_b, wgu, wdn, gsend, grecv, gown, hbuf,
    ybuf_a, ybuf_b, r1buf, r2buf, rbuf, yret_a, yret_b, tokb, t1buf, t2buf, zsend, zret,
    pair_sem, z_s, z_r, ya_s, ya_r, yb_s, yb_r, x1_s, x1_r, x2_s, x2_r, b1_s, b1_r, b2_s, b2_r,
    w_l, w_s, w_r, g_s, g_r, h_s, h_r, r1_s, r1_r, r2_s, r2_r, t1_s, t1_r, t2_s, t2_r,
    yra_s, yra_r, yrb_s, yrb_r, zr_s, zr_r, in_sem,
):
    me_e, me_s = lax.axis_index("expert"), lax.axis_index("shard")
    z_lo, y = me_e // 4, lax.rem(me_e, 4)
    z = (me_s // 8) * 2 + z_lo
    x = lax.rem(me_s // 2, 4)
    core = lax.rem(me_s, 2)
    sibling = device_of(x, y, z, 1 - core)
    left = device_of(lax.rem(x + 3, 4), y, z, core)
    right = device_of(lax.rem(x + 1, 4), y, z, core)

    def at_y(r):
        return device_of(x, lax.rem(y + r, 4), z, core)

    def at_z(d, to_core=core):
        return device_of(x, y, lax.rem(z + d, 8), to_core)

    barrier = pltpu.get_barrier_semaphore()
    greeted = [at_z(d, c) for d in (4, 3, 5, 2, 6, 1, 7) for c in (0, 1)] + [at_y(r) for r in (2, 1, 3)] + [left, right, sibling]
    for device in greeted:
        pl.semaphore_signal(barrier, inc=1, device_id=device, device_id_type=MESH)

    inputs = [
        pltpu.make_async_copy(tok_hbm, tok_ref, in_sem.at[0]),
        pltpu.make_async_copy(gain_hbm, gain_ref, in_sem.at[1]),
        pltpu.make_async_copy(routes_hbm, routes_ref, in_sem.at[2]),
        pltpu.make_async_copy(gates_hbm, gates_ref, in_sem.at[3]),
        pltpu.make_async_copy(cap_hbm, cap_ref, in_sem.at[4]),
    ]
    for copy in inputs:
        copy.start()

    own = 1
    TURNS = (0, 2, 4, 6)

    def place(d):
        return 2 * TURNS.index(d - 1) if d % 2 else 2 * TURNS.index((8 - d) % 8) + 1

    mine = pl.ds(pl.multiple_of(core * HALF, HALF), HALF)
    other = pl.ds(pl.multiple_of((1 - core) * HALF, HALF), HALF)
    local_weights = [
        pltpu.make_async_copy(wg_ref.at[0, mine], wgu.at[2], w_l.at[0]),
        pltpu.make_async_copy(wu_ref.at[0, mine], wgu.at[3], w_l.at[1]),
        pltpu.make_async_copy(wd_ref.at[0, :, mine], wdn.at[0], w_l.at[2]),
    ]
    pair_weights = [
        remote(wg_ref.at[0, other], wgu.at[0], w_s.at[0], w_r.at[0], sibling),
        remote(wu_ref.at[0, other], wgu.at[1], w_s.at[1], w_r.at[1], sibling),
        remote(wd_ref.at[0, :, other], wdn.at[1], w_s.at[2], w_r.at[2], sibling),
    ]
    for copy in local_weights:
        copy.start()

    for copy in inputs:
        copy.wait()
    tokens = tok_ref[...].astype(F32)
    scale = lax.rsqrt(jnp.mean(tokens * tokens, axis=-1, keepdims=True) + 1e-05)
    normed = tokens * scale * gain_ref[...]
    lanes = routing_lanes(columns_of(routes_ref[...]), columns_of(gates_ref[...]), cap_ref)
    first = core == 0
    own_half = jnp.where(first, normed[:, :HALF], normed[:, HALF:])
    pair_src[:, :HALF] = jnp.where(first, normed[:, HALF:], normed[:, :HALF]).astype(BF16)
    pair_src[:, HALF:] = lanes.astype(BF16)

    pl.semaphore_wait(barrier, len(greeted))
    pair = remote(pair_src, pair_dst, pair_sem.at[0], pair_sem.at[1], sibling)
    pair.start()
    for copy in pair_weights:
        copy.start()
    pair.wait_recv()
    their_half = pair_dst[:, :HALF].astype(F32)
    their_lanes = pair_dst[:, HALF:].astype(F32)
    ztok[own, :, :HALF] = jnp.concatenate(
        [jnp.where(first, own_half, their_half), jnp.where(first, their_half, own_half)], axis=0
    ).astype(BF16)
    ztok[own, :, HALF:] = jnp.concatenate(
        [jnp.where(first, lanes, their_lanes), jnp.where(first, their_lanes, lanes)], axis=0
    ).astype(BF16)

    def z_copy(d):
        n = place(d)
        return remote(ztok.at[own], ztok.at[n], z_s.at[n], z_r.at[n], at_z(8 - d))

    for d in (1, 3, 6, 5, 4, 7, 2):
        z_copy(d).start()

    def z_arrival(n):
        return remote(ztok.at[own], ztok.at[n], z_s.at[n], z_r.at[n], at_z(1))

    def weights_of(meta, turned):
        shape = (64, META) if turned else (META, 64)
        lane = lax.broadcasted_iota(jnp.int32, shape, 1 if turned else 0)
        column = lax.broadcasted_iota(jnp.int32, shape, 0 if turned else 1)
        expert = z_lo * 4 + (y + column // 16) % 4
        wanted = expert * 4 + column % 4
        pick = ((lane % 32 == wanted) & (lane < 96)).astype(F32).astype(BF16)
        if turned:
            raw = lax.dot_general(pick, meta, (((1,), (1,)), ((), ())), preferred_element_type=F32)
        else:
            raw = jnp.dot(meta, pick, preferred_element_type=F32)
        shape = (64, 32) if turned else (32, 64)
        column = lax.broadcasted_iota(jnp.int32, shape, 0 if turned else 1)
        row = lax.broadcasted_iota(jnp.int32, shape, 1 if turned else 0)
        return jnp.where(row // 8 == (column // 4) % 4, raw, 0.0)

    def picker_of(meta):
        return jnp.where(weights_of(meta, True) != 0.0, 1.0, 0.0).astype(BF16)

    def picked(picker, slab):
        return jnp.dot(picker, slab, preferred_element_type=F32).astype(BF16).reshape(4, 16, slab.shape[1])

    def combined(weights, rows):
        high = weights.astype(BF16)
        rest = (weights - high.astype(F32)).astype(BF16)
        made = jnp.dot(high, rows, preferred_element_type=F32) + jnp.dot(rest, rows, preferred_element_type=F32)
        return made

    def ya_copy(k, r):
        return remote(sbuf_a.at[k, r - 1], xbuf_a.at[k, 0, 4 - r], ya_s.at[k, r - 1], ya_r.at[k, 3 - r], at_y(r))

    PARTS = ((0, 1), (1, 2), (3, 1))

    def yb_copy(k, part, r):
        rows = pl.ds(*PARTS[part])
        return remote(
            sbuf_b.at[k, r - 1, rows], xbuf_b.at[k, rows, 4 - r], yb_s.at[k, part, r - 1], yb_r.at[k, part, 3 - r], at_y(r)
        )

    def x1_copies(k):
        def copy(way, turn, rows, device):
            return remote(
                xbuf_a.at[k, 0, rows], xbuf_a.at[k, 1 + way, rows], x1_s.at[k, way, turn], x1_r.at[k, way, turn], device
            )

        return copy(0, 0, LOW, right), copy(1, 0, HIGH, left), copy(0, 1, HIGH, right), copy(1, 1, LOW, left)

    def x2_copies(k):
        return (
            remote(xbuf_a.at[k, 1, LOW], xbuf_a.at[k, 3, LOW], x2_s.at[k, 0], x2_r.at[k, 0], right),
            remote(xbuf_a.at[k, 2, HIGH], xbuf_a.at[k, 3, HIGH], x2_s.at[k, 1], x2_r.at[k, 1], left),
        )

    def b1_copies(k):
        def copy(way, turn, n, device):
            return remote(
                ztok.at[2 * k + n, :, A:], xtok.at[k, way, n], b1_s.at[k, way, turn], b1_r.at[k, way, turn], device
            )

        return copy(0, 0, 0, right), copy(1, 0, 1, left), copy(0, 1, 1, right), copy(1, 1, 0, left)

    def b2_copies(k):
        return (
            remote(xtok.at[k, 0, 0], xtok.at[k, 2, 0], b2_s.at[k, 0], b2_r.at[k, 0], right),
            remote(xtok.at[k, 1, 1], xtok.at[k, 2, 1], b2_s.at[k, 1], b2_r.at[k, 1], left),
        )

    def dispatch(k):
        z_arrival(2 * k).wait_recv()

        if k > 0:
            z_arrival(2 * k + 1).wait_recv()
        for copy in b1_copies(k):
            copy.start()
        picker = picker_of(ztok[pl.ds(2 * k, 2), :, HALF:].reshape(32, META))

        def slots_at(start, width):
            return picked(picker, ztok[pl.ds(2 * k, 2), :, start : start + width].reshape(32, width))

        for start, width in tiles_of(A):
            slots = slots_at(start, width)
            xbuf_a[k, 0, 0, :, start : start + width] = slots[0]
            sbuf_a[k, :, :, start : start + width] = slots[1:]
        for r in (2, 1, 3):
            ya_copy(k, r).start()
        for start, width in tiles_of(B):
            slots = slots_at(A + start, width)
            xbuf_b[k, 0, 0, :, start : start + width] = slots[0]
            sbuf_b[k, :, 0, :, start : start + width] = slots[1:]
        for r in (2, 1, 3):
            yb_copy(k, 0, r).start()

    def dispatch_from(k, rel):
        picker = picker_of(xtok[k, rel - 1, :, :, B:].reshape(32, META))
        for start, width in tiles_of(B):
            slots = picked(picker, xtok[k, rel - 1, :, :, start : start + width].reshape(32, width))
            xbuf_b[k, rel, 0, :, start : start + width] = slots[0]
            sbuf_b[k, :, rel, :, start : start + width] = slots[1:]

    def pass_tokens(k):
        for near, far in zip(b1_copies(k), b2_copies(k)):
            near.wait_recv()
            far.start()

    def ring_slots(k):
        for r in (1, 3, 2):
            ya_copy(k, r).wait_recv()
        for copy in x1_copies(k):
            copy.start()

    def dispatch_near(k):
        for copy in b1_copies(k)[2:]:
            copy.wait_recv()

        @pl.loop(1, 3)
        def _(rel):
            dispatch_from(k, rel)

        for r in (2, 1, 3):
            yb_copy(k, 1, r).start()

    def dispatch_far(k):
        for copy in b2_copies(k):
            copy.wait_recv()
        dispatch_from(k, 3)
        for r in (2, 1, 3):
            yb_copy(k, 2, r).start()

    def pass_slots(k):
        for near, far in zip(x1_copies(k), x2_copies(k)):
            near.wait_recv()
            far.start()

    def pre_activations(k):
        return remote(gsend.at[k], grecv.at[k], g_s.at[k], g_r.at[k], sibling)

    def hidden_copy(k):
        return remote(hbuf.at[k, 0], hbuf.at[k, 1], h_s.at[k], h_r.at[k], sibling)

    def r1_copies(k):
        return (
            remote(ybuf_a.at[k, 3, LOW], r1buf.at[k, 0], r1_s.at[k, 0], r1_r.at[k, 0], left),
            remote(ybuf_a.at[k, 3, HIGH], r1buf.at[k, 1], r1_s.at[k, 1], r1_r.at[k, 1], right),
        )

    def r2_copies(k):
        def copy(way, turn, rows, device):
            return remote(
                ybuf_a.at[k, 1 + way, rows], r2buf.at[k, 1 - way, rows], r2_s.at[k, way, turn], r2_r.at[k, way, turn], device
            )

        return copy(0, 0, HIGH, left), copy(1, 0, LOW, right), copy(0, 1, LOW, left), copy(1, 1, HIGH, right)

    def yra_copy(k, i):
        return remote(rbuf.at[k, i - 1], yret_a.at[k, 4 - i], yra_s.at[k, i - 1], yra_r.at[k, 3 - i], at_y(i))

    RETURNS = ((3, 1), (0, 3))

    def yrb_copy(k, part, i):
        rows = pl.ds(*RETURNS[part])
        return remote(
            ybuf_b.at[k, rows, i], yret_b.at[k, rows, 3 - i], yrb_s.at[k, part, i - 1], yrb_r.at[k, part, 3 - i], at_y(i)
        )

    def t1_copies(k):
        return (
            remote(tokb.at[k, 3, 0], t1buf.at[k, 0], t1_s.at[k, 0], t1_r.at[k, 0], left),
            remote(tokb.at[k, 3, 1], t1buf.at[k, 1], t1_s.at[k, 1], t1_r.at[k, 1], right),
        )

    def t2_copies(k):
        def copy(way, turn, n, device):
            return remote(
                tokb.at[k, 1 + way, n], t2buf.at[k, 1 - way, n], t2_s.at[k, way, turn], t2_r.at[k, way, turn], device
            )

        return copy(0, 0, 1, left), copy(1, 0, 0, right), copy(0, 1, 0, left), copy(1, 1, 1, right)

    def expert_hidden(k):
        if k == FIRST:
            for copy in local_weights:
                copy.wait()
            for copy in pair_weights:
                copy.wait_recv()
        for copy in x1_copies(k)[2:] + x2_copies(k):
            copy.wait_recv()
        for part in range(3):
            for r in (1, 3, 2):
                yb_copy(k, part, r).wait_recv()

        def project(n):
            made = jnp.dot(xbuf_a[k].reshape(256, A), wgu[n, :A], preferred_element_type=F32)
            return made + jnp.dot(xbuf_b[k].reshape(256, B), wgu[n, A:], preferred_element_type=F32)

        @pl.loop(0, 2)
        def _(n):
            gsend[k, n] = project(n)

        pre_activations(k).start()

        @pl.loop(0, 2)
        def _(n):
            gown[n] = project(n + 2)

        pre_activations(k).wait_recv()
        gate = gown[0] + grecv[k, 0]
        up = gown[1] + grecv[k, 1]
        hbuf[k, 0] = (gate / (1.0 + jnp.exp(-gate)) * up).astype(BF16)
        hidden_copy(k).start()

    def expert_out(k):
        hidden_copy(k).wait_recv()

        def outputs(start, width):
            columns = slice(start, start + width)
            made = jnp.dot(hbuf[k, 0], wdn[0, :, columns], preferred_element_type=F32)
            made = made + jnp.dot(hbuf[k, 1], wdn[1, :, columns], preferred_element_type=F32)
            return made.astype(BF16).reshape(4, 4, 16, width)

        for start, width in tiles_of(B):
            ybuf_b[k, :, :, :, start : start + width] = outputs(A + start, width)
        for part in range(2):
            for i in (2, 1, 3):
                yrb_copy(k, part, i).start()
        for start, width in tiles_of(A):
            ybuf_a[k, :, :, :, start : start + width] = outputs(start, width)
        for copy in r1_copies(k) + r2_copies(k)[:2]:
            copy.start()

    def plus(ref, *others):
        total = ref[...].astype(F32)
        for term in others:
            total = total + term[...].astype(F32)
        return total.astype(BF16)

    def sum_slots(k):
        for copy in r1_copies(k):
            copy.wait_recv()
        ybuf_a[k, 1, 0:2] = plus(ybuf_a.at[k, 1, 0:2], r1buf.at[k, 0])
        ybuf_a[k, 2, 2:4] = plus(ybuf_a.at[k, 2, 2:4], r1buf.at[k, 1])
        for copy in r2_copies(k)[2:]:
            copy.start()

    def combine_for(k, rel, meta):
        weights = weights_of(meta.reshape(32, META), False)
        for start, width in tiles_of(B):
            columns = slice(start, start + width)
            rows = jnp.concatenate([ybuf_b[k, rel, 0, :, columns][None], yret_b[k, rel, :, :, columns]], axis=0)
            tokb[k, rel, :, :, columns] = combined(weights, rows.reshape(64, width)).astype(BF16).reshape(2, 16, width)

    def combine_far(k):
        for i in (1, 3, 2):
            yrb_copy(k, 0, i).wait_recv()
        combine_for(k, 3, xtok[k, 2, :, :, B:])
        for copy in t1_copies(k):
            copy.start()

    def combine_near(k):
        for i in (1, 3, 2):
            yrb_copy(k, 1, i).wait_recv()

        @pl.loop(1, 3)
        def _(rel):
            combine_for(k, rel, xtok[k, rel - 1, :, :, B:])

        for copy in t2_copies(k)[:2]:
            copy.start()
        combine_for(k, 0, ztok[pl.ds(2 * k, 2), :, HALF:])

    def sum_tokens(k):
        for copy in t1_copies(k):
            copy.wait_recv()
        tokb[k, 1, 0] = plus(tokb.at[k, 1, 0], t1buf.at[k, 0])
        tokb[k, 2, 1] = plus(tokb.at[k, 2, 1], t1buf.at[k, 1])
        for copy in t2_copies(k)[2:]:
            copy.start()

    def return_slots(k):
        for copy in r2_copies(k):
            copy.wait_recv()
        total = plus(ybuf_a.at[k, 0], r2buf.at[k, 0], r2buf.at[k, 1])
        yret_a[k, 0] = total[0]
        rbuf[k] = total[1:]
        for i in (2, 1, 3):
            yra_copy(k, i).start()

    def zr_copy(n, d, c):
        return remote(zsend.at[n, c], zret.at[n, core], zr_s.at[n, c], zr_r.at[n, core], at_z(d, c))

    def zr_sibling():
        return remote(zsend.at[own, 1 - core], zret.at[own, core], zr_s.at[own, 1 - core], zr_r.at[own, core], sibling)

    def zr_arrival(n, h):
        return remote(zsend.at[n, 0], zret.at[n, h], zr_s.at[n, 0], zr_r.at[n, h], at_z(1))

    def combine(k):
        for copy in t2_copies(k):
            copy.wait_recv()
        total = tokb[k, 0].astype(F32) + t2buf[k, 0].astype(F32) + t2buf[k, 1].astype(F32)
        zsend[pl.ds(2 * k, 2), :, :, A:] = total.reshape(2, 2, 8, B).astype(BF16)
        for r in (1, 3, 2):
            yra_copy(k, r).wait_recv()
        weights = weights_of(ztok[pl.ds(2 * k, 2), :, HALF:].reshape(32, META), False)
        for start, width in tiles_of(A):
            columns = slice(start, start + width)
            made = combined(weights, yret_a[k, :, :, columns].reshape(64, width))
            zsend[pl.ds(2 * k, 2), :, :, columns] = made.reshape(2, 2, 8, width).astype(BF16)
        for c in (0, 1):
            zr_copy(2 * k, TURNS[k] + 1, c).start()
        if k > 0:
            for c in (0, 1):
                zr_copy(2 * k + 1, 8 - TURNS[k], c).start()
        else:
            zr_sibling().start()
            zret[own, core] = zsend[own, core]

    stages = {
        "d": dispatch,
        "nb": pass_tokens,
        "na": ring_slots,
        "nd": dispatch_near,
        "fb": dispatch_far,
        "fa": pass_slots,
        "h": expert_hidden,
        "o": expert_out,
        "Na": sum_slots,
        "Nc": combine_far,
        "Nb": combine_near,
        "Rb": sum_tokens,
        "Ra": return_slots,
        "C": combine,
    }
    for name in ORDER:
        stages[name[:-1]](int(name[-1]))

    pair.wait_send()
    for copy in pair_weights:
        copy.wait_send()
    for d in range(1, 8):
        z_copy(d).wait_send()

    def sent(k, carry):
        for r in (1, 2, 3):
            ya_copy(k, r).wait_send()
            yra_copy(k, r).wait_send()
            for part in range(2):
                yrb_copy(k, part, r).wait_send()
            for part in range(3):
                yb_copy(k, part, r).wait_send()
        for copies in (x1_copies, x2_copies, b1_copies, b2_copies, r1_copies, r2_copies, t1_copies, t2_copies):
            for copy in copies(k):
                copy.wait_send()
        pre_activations(k).wait_send()
        hidden_copy(k).wait_send()
        return carry

    lax.fori_loop(0, CHUNKS, sent, 0)

    totals = [jnp.zeros((8, HALF), F32)] * 2
    for k in [int(name[1:]) for name in ORDER if name[0] == "C"]:
        for n in (2 * k, 2 * k + 1):
            if n == own:
                remote(
                    zsend.at[own, 0], zret.at[own, 1 - core], zr_s.at[own, 0], zr_r.at[own, 1 - core], sibling
                ).wait_recv()
            for h in (0, 1):
                if n != own:
                    zr_arrival(n, h).wait_recv()
                totals[h] = totals[h] + zret[n, h].astype(F32)
    for h in (0, 1):
        out_ref[:, h * HALF : (h + 1) * HALF] = totals[h].astype(BF16)
    zr_sibling().wait_send()
    for n in (0, 2, 3, 4, 5, 6, 7):
        for c in (0, 1):
            zr_copy(n, 1, c).wait_send()


def on_device(tokens, norm_gain, routes, gate_weights, capacity, w_gate, w_up, w_down):
    vmem = pl.BlockSpec(memory_space=pltpu.VMEM)
    whole = pl.BlockSpec(memory_space=pl.ANY)
    k = CHUNKS

    def held(*shape, dtype=BF16):
        return pltpu.VMEM(shape, dtype)

    def sems(*shape):
        return [pltpu.SemaphoreType.DMA(shape)]

    return pl.pallas_call(
        kernel,
        out_shape=jax.ShapeDtypeStruct((8, D), BF16),
        in_specs=[whole] * 8,
        out_specs=vmem,
        scratch_shapes=[
            held(8, D),
            held(1, D, dtype=F32),
            held(2, 8, dtype=jnp.int32),
            held(2, 8, dtype=F32),
            pltpu.SMEM((8,), jnp.int32),
            held(8, HALF + META),
            held(8, HALF + META),
            held(8, 16, HALF + META),
            held(k, 3, 16, A),
            held(k, 3, 4, 16, B),
            held(k, 3, 2, 16, B + META),
            held(k, 4, 4, 16, A),
            held(k, 4, 4, 16, B),
            held(4, HALF, FW),
            held(2, FW, HALF),
            held(k, 2, 256, FW, dtype=F32),
            held(k, 2, 256, FW, dtype=F32),
            held(2, 256, FW, dtype=F32),
            held(k, 2, 256, FW),
            held(k, 4, 4, 16, A),
            held(k, 4, 4, 16, B),
            held(k, 2, 2, 16, A),
            held(k, 2, 4, 16, A),
            held(k, 3, 16, A),
            held(k, 4, 16, A),
            held(k, 4, 3, 16, B),
            held(k, 4, 2, 16, B),
            held(k, 2, 16, B),
            held(k, 2, 2, 16, B),
            held(8, 2, 8, HALF),
            held(8, 2, 8, HALF),
        ]
        + sems(2)
        + sems(8) * 2
        + sems(k, 3) * 2
        + sems(k, 3, 3) * 2
        + (sems(k, 2, 2) * 2 + sems(k, 2) * 2) * 2
        + sems(3) * 3
        + sems(k) * 4
        + (sems(k, 2) * 2 + sems(k, 2, 2) * 2) * 2
        + sems(k, 3) * 2
        + sems(k, 2, 3) * 2
        + sems(8, 2) * 2
        + sems(5),
        compiler_params=pltpu.CompilerParams(
            collective_id=0, has_side_effects=True, vmem_limit_bytes=67043328
        ),
    )(tokens, norm_gain[None], routes.T, gate_weights.T, capacity, w_gate, w_up, w_down)


def solution(mesh):
    in_specs = (
        P(("expert", "shard"), None),
        P(),
        P(("expert", "shard"), None),
        P(("expert", "shard"), None),
        P(),
        P("expert", None, "shard"),
        P("expert", None, "shard"),
        P("expert", "shard", None),
    )
    out_specs = P(("expert", "shard"), None)
    return jax.shard_map(
        on_device, mesh=mesh, in_specs=in_specs, out_specs=out_specs, check_vma=False
    )
```

```python
import jax
import jax.numpy as jnp
from jax import lax
from jax.experimental import pallas as pl
from jax.experimental.pallas import tpu as pltpu
from jax.sharding import PartitionSpec as P

MESH = pl.DeviceIdType.MESH
F32, BF16 = jnp.float32, jnp.bfloat16

D = 6144
HALF = D // 2
FW = 256
META = 128
CHUNKS = 4
A = 1664
B = HALF - A
TILE = 256
LOW, HIGH = pl.ds(0, 2), pl.ds(2, 2)
ORDER = (
    "d0", "nb0", "d1", "nd0", "na0", "nb1", "d2", "fa0", "fb0", "d3", "nb2", "na2", "nd2", "nb3", "fa2", "fb2",
    "nd3", "na3", "nd1", "na1", "h2", "fb3", "fa3", "fb1", "o2", "fa1", "h0", "h3", "Na2", "Nc2", "o3", "h1", "Nb2",
    "Rb2", "Nc3", "Na3", "Ra2", "o1", "Nb3", "Ra3", "Rb3", "o0", "Na1", "C2", "Nc1", "C3", "Na0", "Nc0", "Nb1",
    "Ra1", "Rb1", "Ra0", "Nb0", "Rb0", "C1", "C0",
)
FIRST = 2


def tiles_of(width):
    return [(start, min(TILE, width - start)) for start in range(0, width, TILE)]


def device_of(x, y, z, core):
    return (lax.rem(z, 2) * 4 + y, (z // 2) * 8 + x * 2 + core)


def remote(src, dst, send, recv, device):
    return pltpu.make_async_remote_copy(
        src_ref=src,
        dst_ref=dst,
        send_sem=send,
        recv_sem=recv,
        device_id=device,
        device_id_type=MESH,
    )


def columns_of(pair):
    row = lax.broadcasted_iota(jnp.int32, (8, 8), 0)
    lane = lax.broadcasted_iota(jnp.int32, (8, 8), 1)
    spread = [jnp.broadcast_to(pair[k : k + 1, :], (8, 8)) for k in range(2)]
    zero = jnp.zeros((8, 8), pair.dtype)
    return [jnp.sum(jnp.where(row == lane, s, zero), axis=1, keepdims=True) for s in spread]


def routing_lanes(routes, gates, cap_ref):
    lane = lax.broadcasted_iota(jnp.int32, (8, META), 1)
    row = lax.broadcasted_iota(jnp.int32, (8, META), 0)
    expert, slot = lane // 4, lane % 4
    named = [routes[k] == expert for k in range(2)]
    either = (named[0] | named[1]).astype(jnp.int32)
    running = either
    for shift in (1, 2, 4):
        running = running + jnp.where(row >= shift, pltpu.roll(running, shift, 0), 0)
    rank = running - either
    limit = jnp.zeros((8, META), jnp.int32)
    for e in range(8):
        limit = jnp.where(expert == e, cap_ref[e], limit)
    held = (rank == slot) & (rank < limit)
    weights = jnp.zeros((8, META), F32)
    for k in range(2):
        weights = weights + jnp.where(named[k] & held, gates[k], 0.0)
    high = weights.astype(BF16).astype(F32)
    middle = (weights - high).astype(BF16).astype(F32)
    low = weights - high - middle
    return high + pltpu.roll(middle, 32, 1) + pltpu.roll(low, 64, 1)


def kernel(
    tok_hbm, gain_hbm, routes_hbm, gates_hbm, cap_hbm, wg_ref, wu_ref, wd_ref, out_ref,
    tok_ref, gain_ref, routes_ref, gates_ref, cap_ref,
    ztok_src, ztok, sbuf_a, sbuf_b, xtok, xbuf_a, xbuf_b, wgu, wdn, gsend, grecv, gown, hbuf,
    ybuf_a, ybuf_b, r1buf, r2buf, rbuf, yret_a, yret_b, tokb, t1buf, t2buf, zsend, zret,
    z_s, z_r, ya_s, ya_r, yb_s, yb_r, x1_s, x1_r, x2_s, x2_r, b1_s, b1_r, b2_s, b2_r,
    w_l, w_s, w_r, g_s, g_r, h_s, h_r, r1_s, r1_r, r2_s, r2_r, t1_s, t1_r, t2_s, t2_r,
    yra_s, yra_r, yrb_s, yrb_r, zr_s, zr_r, in_sem,
):
    me_e, me_s = lax.axis_index("expert"), lax.axis_index("shard")
    z_lo, y = me_e // 4, lax.rem(me_e, 4)
    z = (me_s // 8) * 2 + z_lo
    x = lax.rem(me_s // 2, 4)
    core = lax.rem(me_s, 2)
    sibling = device_of(x, y, z, 1 - core)
    left = device_of(lax.rem(x + 3, 4), y, z, core)
    right = device_of(lax.rem(x + 1, 4), y, z, core)

    def at_y(r):
        return device_of(x, lax.rem(y + r, 4), z, core)

    def at_z(d, to_core=core):
        return device_of(x, y, lax.rem(z + d, 8), to_core)

    barrier = pltpu.get_barrier_semaphore()
    greeted = [at_z(d, c) for d in (4, 3, 5, 2, 6, 1, 7) for c in (0, 1)] + [at_y(r) for r in (2, 1, 3)] + [left, right, sibling]
    for device in greeted:
        pl.semaphore_signal(barrier, inc=1, device_id=device, device_id_type=MESH)

    inputs = [
        pltpu.make_async_copy(tok_hbm, tok_ref, in_sem.at[0]),
        pltpu.make_async_copy(gain_hbm, gain_ref, in_sem.at[1]),
        pltpu.make_async_copy(routes_hbm, routes_ref, in_sem.at[2]),
        pltpu.make_async_copy(gates_hbm, gates_ref, in_sem.at[3]),
        pltpu.make_async_copy(cap_hbm, cap_ref, in_sem.at[4]),
    ]
    for copy in inputs:
        copy.start()

    own = 1
    TURNS = (0, 6, 4, 2)

    def place(d):
        return 2 * TURNS.index(d - 1) if d % 2 else 2 * TURNS.index((8 - d) % 8) + 1

    mine = pl.ds(pl.multiple_of(core * HALF, HALF), HALF)
    other = pl.ds(pl.multiple_of((1 - core) * HALF, HALF), HALF)
    local_weights = [
        pltpu.make_async_copy(wg_ref.at[0, mine], wgu.at[2], w_l.at[0]),
        pltpu.make_async_copy(wu_ref.at[0, mine], wgu.at[3], w_l.at[1]),
        pltpu.make_async_copy(wd_ref.at[0, :, mine], wdn.at[0], w_l.at[2]),
    ]
    pair_weights = [
        remote(wg_ref.at[0, other], wgu.at[0], w_s.at[0], w_r.at[0], sibling),
        remote(wu_ref.at[0, other], wgu.at[1], w_s.at[1], w_r.at[1], sibling),
        remote(wd_ref.at[0, :, other], wdn.at[1], w_s.at[2], w_r.at[2], sibling),
    ]
    for copy in local_weights:
        copy.start()

    for copy in inputs:
        copy.wait()
    tokens = tok_ref[...].astype(F32)
    scale = lax.rsqrt(jnp.mean(tokens * tokens, axis=-1, keepdims=True) + 1e-05)
    normed = tokens * scale * gain_ref[...]
    lanes = routing_lanes(columns_of(routes_ref[...]), columns_of(gates_ref[...]), cap_ref)
    for c in (0, 1):
        ztok_src[c, :, :HALF] = normed[:, c * HALF : (c + 1) * HALF].astype(BF16)
        ztok_src[c, :, HALF:] = lanes.astype(BF16)

    def z_copy(d, c):
        n = place(d)
        return remote(ztok_src.at[c], ztok.at[n, core], z_s.at[n, c], z_r.at[n, core], at_z(8 - d, c))

    def z_sibling(slot):
        return remote(ztok_src.at[1 - core], ztok.at[own, slot], z_s.at[own, 0], z_r.at[own, slot], sibling)

    def z_arrival(n, h):
        return remote(ztok_src.at[0], ztok.at[n, h], z_s.at[n, 0], z_r.at[n, h], at_z(1))

    pl.semaphore_wait(barrier, len(greeted))
    z_sibling(core).start()
    for d in (1, 7, 2, 5, 4, 3, 6):
        for c in (0, 1):
            z_copy(d, c).start()
    for copy in pair_weights:
        copy.start()
    ztok[own, core] = ztok_src[core]

    def flat(rows):
        return rows.astype(F32).reshape(32, rows.shape[-1]).astype(BF16)

    def weights_of(meta, turned):
        shape = (64, META) if turned else (META, 64)
        lane = lax.broadcasted_iota(jnp.int32, shape, 1 if turned else 0)
        column = lax.broadcasted_iota(jnp.int32, shape, 0 if turned else 1)
        expert = z_lo * 4 + (y + column // 16) % 4
        wanted = expert * 4 + column % 4
        pick = ((lane % 32 == wanted) & (lane < 96)).astype(F32).astype(BF16)
        if turned:
            raw = lax.dot_general(pick, meta, (((1,), (1,)), ((), ())), preferred_element_type=F32)
        else:
            raw = jnp.dot(meta, pick, preferred_element_type=F32)
        shape = (64, 32) if turned else (32, 64)
        column = lax.broadcasted_iota(jnp.int32, shape, 0 if turned else 1)
        row = lax.broadcasted_iota(jnp.int32, shape, 1 if turned else 0)
        return jnp.where(row // 8 == (column // 4) % 4, raw, 0.0)

    def picker_of(meta):
        return jnp.where(weights_of(meta, True) != 0.0, 1.0, 0.0).astype(BF16)

    def picked(picker, slab):
        return jnp.dot(picker, slab, preferred_element_type=F32).astype(BF16).reshape(4, 16, slab.shape[1])

    def combined(weights, rows):
        high = weights.astype(BF16)
        rest = (weights - high.astype(F32)).astype(BF16)
        made = jnp.dot(high, rows, preferred_element_type=F32) + jnp.dot(rest, rows, preferred_element_type=F32)
        return made

    def ya_copy(k, r):
        return remote(sbuf_a.at[k, r - 1], xbuf_a.at[k, 0, 4 - r], ya_s.at[k, r - 1], ya_r.at[k, 3 - r], at_y(r))

    PARTS = ((0, 1), (1, 2), (3, 1))

    def yb_copy(k, part, r):
        rows = pl.ds(*PARTS[part])
        return remote(
            sbuf_b.at[k, r - 1, rows], xbuf_b.at[k, rows, 4 - r], yb_s.at[k, part, r - 1], yb_r.at[k, part, 3 - r], at_y(r)
        )

    def x1_copies(k):
        def copy(way, turn, rows, device):
            return remote(
                xbuf_a.at[k, 0, rows], xbuf_a.at[k, 1 + way, rows], x1_s.at[k, way, turn], x1_r.at[k, way, turn], device
            )

        return copy(0, 0, LOW, right), copy(1, 0, HIGH, left), copy(0, 1, HIGH, right), copy(1, 1, LOW, left)

    def x2_copies(k):
        return (
            remote(xbuf_a.at[k, 1, LOW], xbuf_a.at[k, 3, LOW], x2_s.at[k, 0], x2_r.at[k, 0], right),
            remote(xbuf_a.at[k, 2, HIGH], xbuf_a.at[k, 3, HIGH], x2_s.at[k, 1], x2_r.at[k, 1], left),
        )

    def b1_copies(k):
        def copy(way, turn, n, device):
            return remote(
                ztok.at[2 * k + n, :, :, A:], xtok.at[k, way, n], b1_s.at[k, way, turn], b1_r.at[k, way, turn], device
            )

        return copy(0, 0, 0, right), copy(1, 0, 1, left), copy(0, 1, 1, right), copy(1, 1, 0, left)

    def b2_copies(k):
        return (
            remote(xtok.at[k, 0, 0], xtok.at[k, 2, 0], b2_s.at[k, 0], b2_r.at[k, 0], right),
            remote(xtok.at[k, 1, 1], xtok.at[k, 2, 1], b2_s.at[k, 1], b2_r.at[k, 1], left),
        )

    def dispatch(k):
        for h in (0, 1):
            z_arrival(2 * k, h).wait_recv()
        if k > 0:
            for h in (0, 1):
                z_arrival(2 * k + 1, h).wait_recv()
        else:
            z_sibling(1 - core).wait_recv()
        for copy in b1_copies(k):
            copy.start()
        picker = picker_of(flat(ztok[pl.ds(2 * k, 2), :, :, HALF:]))

        def slots_at(start, width):
            return picked(picker, flat(ztok[pl.ds(2 * k, 2), :, :, start : start + width]))

        for start, width in tiles_of(A):
            slots = slots_at(start, width)
            xbuf_a[k, 0, 0, :, start : start + width] = slots[0]
            sbuf_a[k, :, :, start : start + width] = slots[1:]
        for r in (2, 1, 3):
            ya_copy(k, r).start()
        for start, width in tiles_of(B):
            slots = slots_at(A + start, width)
            xbuf_b[k, 0, 0, :, start : start + width] = slots[0]
            sbuf_b[k, :, 0, :, start : start + width] = slots[1:]
        for r in (2, 1, 3):
            yb_copy(k, 0, r).start()

    def dispatch_from(k, rel):
        picker = picker_of(flat(xtok[k, rel - 1, :, :, :, B:]))
        for start, width in tiles_of(B):
            slots = picked(picker, flat(xtok[k, rel - 1, :, :, :, start : start + width]))
            xbuf_b[k, rel, 0, :, start : start + width] = slots[0]
            sbuf_b[k, :, rel, :, start : start + width] = slots[1:]

    def pass_tokens(k):
        for near, far in zip(b1_copies(k), b2_copies(k)):
            near.wait_recv()
            far.start()

    def ring_slots(k):
        for r in (1, 3, 2):
            ya_copy(k, r).wait_recv()
        for copy in x1_copies(k):
            copy.start()

    def dispatch_near(k):
        for copy in b1_copies(k)[2:]:
            copy.wait_recv()

        @pl.loop(1, 3)
        def _(rel):
            dispatch_from(k, rel)

        for r in (2, 1, 3):
            yb_copy(k, 1, r).start()

    def dispatch_far(k):
        for copy in b2_copies(k):
            copy.wait_recv()
        dispatch_from(k, 3)
        for r in (2, 1, 3):
            yb_copy(k, 2, r).start()

    def pass_slots(k):
        for near, far in zip(x1_copies(k), x2_copies(k)):
            near.wait_recv()
            far.start()

    def pre_activations(k):
        return remote(gsend.at[k], grecv.at[k], g_s.at[k], g_r.at[k], sibling)

    def hidden_copy(k):
        return remote(hbuf.at[k, 0], hbuf.at[k, 1], h_s.at[k], h_r.at[k], sibling)

    def r1_copies(k):
        return (
            remote(ybuf_a.at[k, 3, LOW], r1buf.at[k, 0], r1_s.at[k, 0], r1_r.at[k, 0], left),
            remote(ybuf_a.at[k, 3, HIGH], r1buf.at[k, 1], r1_s.at[k, 1], r1_r.at[k, 1], right),
        )

    def r2_copies(k):
        def copy(way, turn, rows, device):
            return remote(
                ybuf_a.at[k, 1 + way, rows], r2buf.at[k, 1 - way, rows], r2_s.at[k, way, turn], r2_r.at[k, way, turn], device
            )

        return copy(0, 0, HIGH, left), copy(1, 0, LOW, right), copy(0, 1, LOW, left), copy(1, 1, HIGH, right)

    def yra_copy(k, i):
        return remote(rbuf.at[k, i - 1], yret_a.at[k, 4 - i], yra_s.at[k, i - 1], yra_r.at[k, 3 - i], at_y(i))

    RETURNS = ((3, 1), (0, 3))

    def yrb_copy(k, part, i):
        rows = pl.ds(*RETURNS[part])
        return remote(
            ybuf_b.at[k, rows, i], yret_b.at[k, rows, 3 - i], yrb_s.at[k, part, i - 1], yrb_r.at[k, part, 3 - i], at_y(i)
        )

    def t1_copies(k):
        return (
            remote(tokb.at[k, 3, 0], t1buf.at[k, 0], t1_s.at[k, 0], t1_r.at[k, 0], left),
            remote(tokb.at[k, 3, 1], t1buf.at[k, 1], t1_s.at[k, 1], t1_r.at[k, 1], right),
        )

    def t2_copies(k):
        def copy(way, turn, n, device):
            return remote(
                tokb.at[k, 1 + way, n], t2buf.at[k, 1 - way, n], t2_s.at[k, way, turn], t2_r.at[k, way, turn], device
            )

        return copy(0, 0, 1, left), copy(1, 0, 0, right), copy(0, 1, 0, left), copy(1, 1, 1, right)

    def expert_hidden(k):
        if k == FIRST:
            for copy in local_weights:
                copy.wait()
            for copy in pair_weights:
                copy.wait_recv()
        for copy in x1_copies(k)[2:] + x2_copies(k):
            copy.wait_recv()
        for part in range(3):
            for r in (1, 3, 2):
                yb_copy(k, part, r).wait_recv()

        def project(n):
            made = jnp.dot(xbuf_a[k].reshape(256, A), wgu[n, :A], preferred_element_type=F32)
            return made + jnp.dot(xbuf_b[k].reshape(256, B), wgu[n, A:], preferred_element_type=F32)

        @pl.loop(0, 2)
        def _(n):
            gsend[k, n] = project(n)

        pre_activations(k).start()

        @pl.loop(0, 2)
        def _(n):
            gown[n] = project(n + 2)

        pre_activations(k).wait_recv()
        gate = gown[0] + grecv[k, 0]
        up = gown[1] + grecv[k, 1]
        hbuf[k, 0] = (gate / (1.0 + jnp.exp(-gate)) * up).astype(BF16)
        hidden_copy(k).start()

    def expert_out(k):
        hidden_copy(k).wait_recv()

        def outputs(start, width):
            columns = slice(start, start + width)
            made = jnp.dot(hbuf[k, 0], wdn[0, :, columns], preferred_element_type=F32)
            made = made + jnp.dot(hbuf[k, 1], wdn[1, :, columns], preferred_element_type=F32)
            return made.astype(BF16).reshape(4, 4, 16, width)

        for start, width in tiles_of(B):
            ybuf_b[k, :, :, :, start : start + width] = outputs(A + start, width)
        for part in range(2):
            for i in (2, 1, 3):
                yrb_copy(k, part, i).start()
        for start, width in tiles_of(A):
            ybuf_a[k, :, :, :, start : start + width] = outputs(start, width)
        for copy in r1_copies(k) + r2_copies(k)[:2]:
            copy.start()

    def plus(ref, *others):
        total = ref[...].astype(F32)
        for term in others:
            total = total + term[...].astype(F32)
        return total.astype(BF16)

    def sum_slots(k):
        for copy in r1_copies(k):
            copy.wait_recv()
        ybuf_a[k, 1, 0:2] = plus(ybuf_a.at[k, 1, 0:2], r1buf.at[k, 0])
        ybuf_a[k, 2, 2:4] = plus(ybuf_a.at[k, 2, 2:4], r1buf.at[k, 1])
        for copy in r2_copies(k)[2:]:
            copy.start()

    def combine_for(k, rel, meta):
        weights = weights_of(flat(meta), False)
        for start, width in tiles_of(B):
            columns = slice(start, start + width)
            rows = jnp.concatenate([ybuf_b[k, rel, 0, :, columns][None], yret_b[k, rel, :, :, columns]], axis=0)
            tokb[k, rel, :, :, columns] = combined(weights, rows.reshape(64, width)).astype(BF16).reshape(2, 16, width)

    def combine_far(k):
        for i in (1, 3, 2):
            yrb_copy(k, 0, i).wait_recv()
        combine_for(k, 3, xtok[k, 2, :, :, :, B:])
        for copy in t1_copies(k):
            copy.start()

    def combine_near(k):
        for i in (1, 3, 2):
            yrb_copy(k, 1, i).wait_recv()

        @pl.loop(1, 3)
        def _(rel):
            combine_for(k, rel, xtok[k, rel - 1, :, :, :, B:])

        for copy in t2_copies(k)[:2]:
            copy.start()
        combine_for(k, 0, ztok[pl.ds(2 * k, 2), :, :, HALF:])

    def sum_tokens(k):
        for copy in t1_copies(k):
            copy.wait_recv()
        tokb[k, 1, 0] = plus(tokb.at[k, 1, 0], t1buf.at[k, 0])
        tokb[k, 2, 1] = plus(tokb.at[k, 2, 1], t1buf.at[k, 1])
        for copy in t2_copies(k)[2:]:
            copy.start()

    def return_slots(k):
        for copy in r2_copies(k):
            copy.wait_recv()
        total = plus(ybuf_a.at[k, 0], r2buf.at[k, 0], r2buf.at[k, 1])
        yret_a[k, 0] = total[0]
        rbuf[k] = total[1:]
        for i in (2, 1, 3):
            yra_copy(k, i).start()

    def zr_copy(n, d, c):
        return remote(zsend.at[n, c], zret.at[n, core], zr_s.at[n, c], zr_r.at[n, core], at_z(d, c))

    def zr_sibling():
        return remote(zsend.at[own, 1 - core], zret.at[own, core], zr_s.at[own, 1 - core], zr_r.at[own, core], sibling)

    def zr_arrival(n, h):
        return remote(zsend.at[n, 0], zret.at[n, h], zr_s.at[n, 0], zr_r.at[n, h], at_z(1))

    def combine(k):
        for copy in t2_copies(k):
            copy.wait_recv()
        total = tokb[k, 0].astype(F32) + t2buf[k, 0].astype(F32) + t2buf[k, 1].astype(F32)
        zsend[pl.ds(2 * k, 2), :, :, A:] = total.reshape(2, 2, 8, B).astype(BF16)
        for r in (1, 3, 2):
            yra_copy(k, r).wait_recv()
        weights = weights_of(flat(ztok[pl.ds(2 * k, 2), :, :, HALF:]), False)
        for start, width in tiles_of(A):
            columns = slice(start, start + width)
            made = combined(weights, yret_a[k, :, :, columns].reshape(64, width))
            zsend[pl.ds(2 * k, 2), :, :, columns] = made.reshape(2, 2, 8, width).astype(BF16)
        for c in (0, 1):
            zr_copy(2 * k, TURNS[k] + 1, c).start()
        if k > 0:
            for c in (0, 1):
                zr_copy(2 * k + 1, 8 - TURNS[k], c).start()
        else:
            zr_sibling().start()
            zret[own, core] = zsend[own, core]

    stages = {
        "d": dispatch,
        "nb": pass_tokens,
        "na": ring_slots,
        "nd": dispatch_near,
        "fb": dispatch_far,
        "fa": pass_slots,
        "h": expert_hidden,
        "o": expert_out,
        "Na": sum_slots,
        "Nc": combine_far,
        "Nb": combine_near,
        "Rb": sum_tokens,
        "Ra": return_slots,
        "C": combine,
    }
    for name in ORDER:
        stages[name[:-1]](int(name[-1]))

    z_sibling(core).wait_send()
    for copy in pair_weights:
        copy.wait_send()
    for d in range(1, 8):
        for c in (0, 1):
            z_copy(d, c).wait_send()

    def sent(k, carry):
        for r in (1, 2, 3):
            ya_copy(k, r).wait_send()
            yra_copy(k, r).wait_send()
            for part in range(2):
                yrb_copy(k, part, r).wait_send()
            for part in range(3):
                yb_copy(k, part, r).wait_send()
        for copies in (x1_copies, x2_copies, b1_copies, b2_copies, r1_copies, r2_copies, t1_copies, t2_copies):
            for copy in copies(k):
                copy.wait_send()
        pre_activations(k).wait_send()
        hidden_copy(k).wait_send()
        return carry

    lax.fori_loop(0, CHUNKS, sent, 0)

    totals = [jnp.zeros((8, HALF), F32)] * 2
    for k in [int(name[1:]) for name in ORDER if name[0] == "C"]:
        for n in (2 * k, 2 * k + 1):
            if n == own:
                remote(
                    zsend.at[own, 0], zret.at[own, 1 - core], zr_s.at[own, 0], zr_r.at[own, 1 - core], sibling
                ).wait_recv()
            for h in (0, 1):
                if n != own:
                    zr_arrival(n, h).wait_recv()
                totals[h] = totals[h] + zret[n, h].astype(F32)
    for h in (0, 1):
        out_ref[:, h * HALF : (h + 1) * HALF] = totals[h].astype(BF16)
    zr_sibling().wait_send()
    for n in (0, 2, 3, 4, 5, 6, 7):
        for c in (0, 1):
            zr_copy(n, 1, c).wait_send()


def on_device(tokens, norm_gain, routes, gate_weights, capacity, w_gate, w_up, w_down):
    vmem = pl.BlockSpec(memory_space=pltpu.VMEM)
    whole = pl.BlockSpec(memory_space=pl.ANY)
    k = CHUNKS

    def held(*shape, dtype=BF16):
        return pltpu.VMEM(shape, dtype)

    def sems(*shape):
        return [pltpu.SemaphoreType.DMA(shape)]

    return pl.pallas_call(
        kernel,
        out_shape=jax.ShapeDtypeStruct((8, D), BF16),
        in_specs=[whole] * 8,
        out_specs=vmem,
        scratch_shapes=[
            held(8, D),
            held(1, D, dtype=F32),
            held(2, 8, dtype=jnp.int32),
            held(2, 8, dtype=F32),
            pltpu.SMEM((8,), jnp.int32),
            held(2, 8, HALF + META),
            held(8, 2, 8, HALF + META),
            held(k, 3, 16, A),
            held(k, 3, 4, 16, B),
            held(k, 3, 2, 2, 8, B + META),
            held(k, 4, 4, 16, A),
            held(k, 4, 4, 16, B),
            held(4, HALF, FW),
            held(2, FW, HALF),
            held(k, 2, 256, FW, dtype=F32),
            held(k, 2, 256, FW, dtype=F32),
            held(2, 256, FW, dtype=F32),
            held(k, 2, 256, FW),
            held(k, 4, 4, 16, A),
            held(k, 4, 4, 16, B),
            held(k, 2, 2, 16, A),
            held(k, 2, 4, 16, A),
            held(k, 3, 16, A),
            held(k, 4, 16, A),
            held(k, 4, 3, 16, B),
            held(k, 4, 2, 16, B),
            held(k, 2, 16, B),
            held(k, 2, 2, 16, B),
            held(8, 2, 8, HALF),
            held(8, 2, 8, HALF),
        ]
        + sems(8, 2) * 2
        + sems(k, 3) * 2
        + sems(k, 3, 3) * 2
        + (sems(k, 2, 2) * 2 + sems(k, 2) * 2) * 2
        + sems(3) * 3
        + sems(k) * 4
        + (sems(k, 2) * 2 + sems(k, 2, 2) * 2) * 2
        + sems(k, 3) * 2
        + sems(k, 2, 3) * 2
        + sems(8, 2) * 2
        + sems(5),
        compiler_params=pltpu.CompilerParams(
            collective_id=0, has_side_effects=True, vmem_limit_bytes=67043328
        ),
    )(tokens, norm_gain[None], routes.T, gate_weights.T, capacity, w_gate, w_up, w_down)


def solution(mesh):
    in_specs = (
        P(("expert", "shard"), None),
        P(),
        P(("expert", "shard"), None),
        P(("expert", "shard"), None),
        P(),
        P("expert", None, "shard"),
        P("expert", None, "shard"),
        P("expert", "shard", None),
    )
    out_specs = P(("expert", "shard"), None)
    return jax.shard_map(
        on_device, mesh=mesh, in_specs=in_specs, out_specs=out_specs, check_vma=False
    )
```
